256 devices in a mesh: gx: 16 (over z, x_lo), gy: 4 (over y), gz: 4 (over x_hi, core).
Axes of the slice: x: 4 (x_hi: 2, x_lo: 2; x = x_hi * 2 + x_lo), y: 4, z: 8, core: 2. Of those that a mesh axis runs over, the one named last changes fastest.
Arguments:
- charges: bfloat16 [64, 16, 16, 32, 128], P('gx', 'gy', 'gz'), may hold values from -6 to 6
- counts: int32 [64, 16, 16], P('gx', 'gy', 'gz'), may hold values from 32 to 128, as said below
- near_offsets: int32 [27, 3], replicated, may hold values from -1 to 1, as said below
- near_blocks: bfloat16 [27, 128, 128], replicated, may hold values from -0.109375 to 0.109375
- leaf_basis: bfloat16 [48, 128], replicated, may hold values from -0.5 to 0.5
- transfer: bfloat16 [8, 48, 48], replicated, may hold values from -0.625 to 0.625
- far_offsets: int32 [2, 32, 3], replicated, may hold values from -2 to 2, as said below
- coupling: bfloat16 [2, 32, 48, 48], replicated, may hold values from -0.15625 to 0.15625
- coarse_coupling: bfloat16 [16, 4, 4, 48, 48], replicated, may hold values from -0.109375 to 0.109375
Outputs:
- potentials: float32 [64, 16, 16, 32, 128], P('gx', 'gy', 'gz')
The draws below stay inside these ranges and needn't reach their ends.
Inputs may be any that keep to these rules, and one draw needn't show every extreme that they name: `counts`: in each device's block of 4 x 4 x 4 leaf boxes some box holds 128 points. `near_offsets`: each of the 27 offsets with components in -1, 0, 1 appears once. `far_offsets`: each level lists 32 distinct offsets whose largest component in magnitude is 2.
All inputs are finite; a program needn't handle non-finite values.
Results may differ from the reference program's by a relative error of at most 0.008.
Values may be sent and summed in bfloat16 or wider, within the bound.
A program may use at most 128 MiB of HBM per device.

```python
import jax
import jax.numpy as jnp
import numpy as np
from jax import lax

PTS = 128
RANK = 48
RHS = 32
STENCIL = 27
LIST = 32
BX = 4
BY = 4
BZ = 4
LX = 64
LY = 16
LZ = 16
CGX = 16
CGY = 4
CGZ = 4


def candidate_table():
    entries = []
    for first in range(-2, 3):
        for second in range(-2, 3):
            for third in range(-2, 3):
                if max(abs(first), abs(second), abs(third)) == 2:
                    entries.append([first, second, third])
    return np.array(entries, dtype=np.int32)


def draw_counts(key, part):
    base = jax.random.randint(jax.random.fold_in(key, 1), (LX, LY, LZ), PTS // 4, PTS + 1)
    chosen = jax.random.randint(jax.random.fold_in(key, 2), (LX // BX, LY // BY, LZ // BZ), 0, BX * BY * BZ)
    spread = jnp.repeat(jnp.repeat(jnp.repeat(chosen, BX, axis=0), BY, axis=1), BZ, axis=2)
    pos_x = (jnp.arange(LX, dtype=jnp.int32) % BX)[:, None, None]
    pos_y = (jnp.arange(LY, dtype=jnp.int32) % BY)[None, :, None]
    pos_z = (jnp.arange(LZ, dtype=jnp.int32) % BZ)[None, None, :]
    within = (pos_x * BY + pos_y) * BZ + pos_z
    return jnp.where(within == spread, PTS, base).astype(jnp.int32)


def draw_near_offsets(key, part):
    order = jax.random.permutation(jax.random.fold_in(key, 3), 27).astype(jnp.int32)
    return jnp.stack([order // 9 - 1, order // 3 % 3 - 1, order % 3 - 1], axis=1).astype(jnp.int32)


def draw_far_offsets(key, part):
    table = jnp.asarray(candidate_table())
    levels = []
    for level in range(2):
        picked = jax.random.permutation(jax.random.fold_in(key, 10 + level), table.shape[0])[:LIST]
        levels.append(table[picked])
    return jnp.stack(levels).astype(jnp.int32)


def block_levels(stream_key, extent, cuts, least, largest):
    factor_of, own = 1.0, jax.random.fold_in(stream_key, 6)
    for position, parts in cuts:
        draws = jnp.exp(jax.random.uniform(jax.random.fold_in(own, position), (parts,), jnp.float32, least / len(cuts), largest / len(cuts)))
        factor_of = factor_of * jnp.repeat(draws, extent[position] // parts).reshape([-1 if axis == position else 1 for axis in range(len(extent))])
    return factor_of


def centred(key, extent, deviation, limit, cuts=(), kind=jnp.bfloat16):
    values = jax.random.normal(key, extent, jnp.float32) * deviation
    if len(cuts) > 0:
        values = block_levels(key, extent, cuts, -0.22, 0.18) * values
    return jnp.clip(values, min=-limit, max=limit).astype(kind)


def setup_inputs(seed: int = 0) -> dict:
    arg_keys = jax.random.split(jax.random.key(seed), 10)
    charges = centred(arg_keys[0], (LX, LY, LZ, RHS, PTS), 1.0, 6.0, ((0, 16), (1, 4), (2, 4)))
    counts = draw_counts(jax.random.fold_in(arg_keys[9], 71), 0)
    near_offsets = draw_near_offsets(jax.random.fold_in(arg_keys[9], 71), 0)
    near_blocks = centred(arg_keys[3], (STENCIL, PTS, PTS), (STENCIL * PTS) ** -0.5, 0.109375)
    leaf_basis = centred(arg_keys[4], (RANK, PTS), PTS ** -0.5, 0.5)
    transfer = centred(arg_keys[5], (8, RANK, RANK), (2 * RANK) ** -0.5, 0.625)
    far_offsets = draw_far_offsets(jax.random.fold_in(arg_keys[9], 71), 0)
    coupling = centred(arg_keys[7], (2, LIST, RANK, RANK), (LIST * RANK) ** -0.5, 0.15625)
    coarse_coupling = centred(arg_keys[8], (CGX, CGY, CGZ, RANK, RANK), (CGX * CGY * CGZ * RANK // 4) ** -0.5, 0.109375)
    return {"charges": charges, "counts": counts, "near_offsets": near_offsets, "near_blocks": near_blocks, "leaf_basis": leaf_basis, "transfer": transfer, "far_offsets": far_offsets, "coupling": coupling, "coarse_coupling": coarse_coupling}


def shifted(field, offset):
    return jnp.roll(field, (-offset[0], -offset[1], -offset[2]), axis=(0, 1, 2))


def upward(moments, transfer):
    first_len, second_len, third_len, rank_count, columns = moments.shape
    split = moments.astype(jnp.float32).reshape(first_len // 2, 2, second_len // 2, 2, third_len // 2, 2, rank_count, columns)
    kids = split.transpose(0, 2, 4, 1, 3, 5, 6, 7).reshape(first_len // 2, second_len // 2, third_len // 2, 8, rank_count, columns)
    return jnp.einsum("ckj,xyzcjr->xyzkr", transfer.astype(jnp.float32), kids).astype(jnp.bfloat16)


def downward(parent, transfer):
    rounded = lax.optimization_barrier(parent.astype(jnp.bfloat16)).astype(jnp.float32)
    kids = jnp.einsum("cjk,xyzjr->xyzckr", transfer.astype(jnp.float32), rounded)
    first_len, second_len, third_len, rank_count, columns = parent.shape
    split = kids.reshape(first_len, second_len, third_len, 2, 2, 2, rank_count, columns)
    return split.transpose(0, 3, 1, 4, 2, 5, 6, 7).reshape(2 * first_len, 2 * second_len, 2 * third_len, rank_count, columns)


def couple_level(moments, offsets, matrices):
    wide = moments.astype(jnp.float32)
    mats = matrices.astype(jnp.float32)

    def step(total, index):
        moved = shifted(wide, offsets[index])
        return total + jnp.einsum("kj,xyzjr->xyzkr", mats[index], moved), None

    start = jnp.zeros(moments.shape, jnp.float32)
    total, unused = lax.scan(step, start, jnp.arange(offsets.shape[0], dtype=jnp.int32))
    return total


def coarse_level(moments, coarse_coupling):
    grid_x, grid_y, grid_z = moments.shape[:3]
    wide = moments.astype(jnp.float32)
    mats = coarse_coupling.astype(jnp.float32)

    def step(total, number):
        off_x = number // (grid_y * grid_z)
        off_y = (number // grid_z) % grid_y
        off_z = number % grid_z
        moved = jnp.roll(wide, (-off_x, -off_y, -off_z), axis=(0, 1, 2))
        return total + jnp.einsum("kj,xyzjr->xyzkr", mats[off_x, off_y, off_z], moved), None

    start = jnp.zeros(moments.shape, jnp.float32)
    total, unused = lax.scan(step, start, jnp.arange(grid_x * grid_y * grid_z, dtype=jnp.int32))
    return total


def reference(charges, counts, near_offsets, near_blocks, leaf_basis, transfer, far_offsets, coupling, coarse_coupling):
    capacity = charges.shape[4]
    live = (jnp.arange(capacity, dtype=jnp.int32) < counts[..., None]).astype(jnp.bfloat16)
    masked = charges * live[:, :, :, None, :]
    masked_wide = masked.astype(jnp.float32)
    blocks = near_blocks.astype(jnp.float32)

    def near_step(total, index):
        moved = shifted(masked_wide, near_offsets[index])
        return total + jnp.einsum("xyzrq,pq->xyzrp", moved, blocks[index]), None

    near, unused = lax.scan(near_step, jnp.zeros(charges.shape, jnp.float32), jnp.arange(near_offsets.shape[0], dtype=jnp.int32))
    basis = leaf_basis.astype(jnp.float32)
    moments_zero = jnp.einsum("kp,xyzrp->xyzkr", basis, masked_wide).astype(jnp.bfloat16)
    moments_one = upward(moments_zero, transfer)
    moments_two = upward(moments_one, transfer)
    local_zero = couple_level(moments_zero, far_offsets[0], coupling[0])
    local_one = couple_level(moments_one, far_offsets[1], coupling[1])
    local_two = coarse_level(moments_two, coarse_coupling)
    total_one = local_one + downward(local_two, transfer)
    total_zero = local_zero + downward(total_one, transfer)
    rounded = lax.optimization_barrier(total_zero.astype(jnp.bfloat16)).astype(jnp.float32)
    far = jnp.einsum("kp,xyzkr->xyzrp", basis, rounded)
    return (near + far) * live[:, :, :, None, :].astype(jnp.float32)
```

```python
import functools

import jax
import jax.numpy as jnp
from jax import lax
from jax.experimental import pallas as pl
from jax.experimental.pallas import tpu as pltpu
from jax.sharding import PartitionSpec as P

MESH = pl.DeviceIdType.MESH
PLANE = [(dx, dz) for dx in (-1, 0, 1) for dz in (-1, 0, 1) if (dx, dz) != (0, 0)]
BF = jnp.bfloat16
F32 = jnp.float32

FIELD_E = ((1, 5, 1), (1, 5, 1), (1, 5, 1))
FIELD_M = ((2, 6, 2), (1, 3, 1), (1, 3, 1))
FIELD_L = ((2, 4, 2), (1, 2, 1), (1, 2, 1))


def source_range(axis, step):
    low, high, width = axis
    if step == 0:
        return pl.ds(low, high - low)
    return pl.ds(high - width, width) if step > 0 else pl.ds(low, width)


def target_range(axis, step):
    low, high, width = axis
    if step == 0:
        return pl.ds(low, high - low)
    return pl.ds(low - width, width) if step > 0 else pl.ds(high, width)


def dot(a, b, contract_a=1, contract_b=0):
    return lax.dot_general(
        a, b, (((contract_a,), (contract_b,)), ((), ())), preferred_element_type=F32
    )


def pack(value):
    zero = jnp.zeros((16, 32), value.dtype)
    return jnp.concatenate([value[0:16], value[16:32], value[32:48], zero], axis=1)


def unpack(value):
    return jnp.concatenate([value[:, 0:32], value[:, 32:64], value[:, 64:96]], axis=0)


def kernel(
    sizes,
    counts,
    near_off,
    far_off,
    charges,
    near_blocks,
    basis_hbm,
    transfer_hbm,
    coupling_hbm,
    coarse_hbm,
    out,
    ext,
    mom,
    one,
    raw,
    blocks,
    basis,
    transfer,
    coupling,
    coarse,
    toep,
    packed,
    near,
    gathered,
    part_out,
    part_in,
    down,
    inverse,
    base,
    in_sem,
    send_sem,
    recv_sem,
    g_send,
    g_recv,
    p_send,
    p_recv,
):
    nx, ny, nz = sizes
    mx, my, mz = lax.axis_index("gx"), lax.axis_index("gy"), lax.axis_index("gz")

    def device(dx, dy, dz):
        return {
            "gx": lax.rem(mx + (dx + nx), nx),
            "gy": lax.rem(my + (dy + ny), ny),
            "gz": lax.rem(mz + (dz + nz), nz),
        }

    loads = [
        pltpu.make_async_copy(src, dst, in_sem.at[i])
        for i, (src, dst) in enumerate(
            (
                (charges, raw),
                (basis_hbm, basis),
                (transfer_hbm, transfer),
                (near_blocks, blocks),
                (coarse_hbm, coarse),
                (coupling_hbm, coupling),
            )
        )
    ]
    for copy in loads:
        copy.start()

    barrier = pltpu.get_barrier_semaphore()
    for dx, dz in PLANE:
        if dx != 0 and dz != 0:
            pl.semaphore_signal(barrier, inc=1, device_id=device(dx, 0, dz), device_id_type=MESH)

    def greet_line(d, carry):
        pl.semaphore_signal(barrier, inc=1, device_id=device(d, 0, 0), device_id_type=MESH)
        return carry

    lax.fori_loop(1, nx, greet_line, 0)

    def greet_plane(d, carry):
        pl.semaphore_signal(
            barrier, inc=1, device_id=device(0, d // nz, d % nz), device_id_type=MESH
        )
        return carry

    lax.fori_loop(1, ny * nz, greet_plane, 0)

    bufs = (ext, mom.at[0], one.at[0])
    fields = (FIELD_E, FIELD_M, FIELD_L)

    def remote(src, dst, sem, target):
        return pltpu.make_async_remote_copy(
            src_ref=src,
            dst_ref=dst,
            send_sem=send_sem.at[sem],
            recv_sem=recv_sem.at[sem],
            device_id=target,
            device_id_type=MESH,
        )

    def plane_copy(f, number):
        dx, dz = PLANE[number]
        ax, ay, az = fields[f]
        mid = source_range(ay, 0)
        return remote(
            bufs[f].at[source_range(ax, dx), mid, source_range(az, dz)],
            bufs[f].at[target_range(ax, dx), mid, target_range(az, dz)],
            18 * f + number,
            device(dx, 0, dz),
        )

    def slab_copy(f, dy, piece):
        ax, ay, az = fields[f]
        full_z = pl.ds(0, az[1] + az[2])
        regions = (
            (source_range(ax, 0), source_range(az, 0)),
            (target_range(ax, 1), full_z),
            (target_range(ax, -1), full_z),
            (source_range(ax, 0), target_range(az, 1)),
            (source_range(ax, 0), target_range(az, -1)),
        )
        rx, rz = regions[piece]
        return remote(
            bufs[f].at[rx, source_range(ay, dy), rz],
            bufs[f].at[rx, target_range(ay, dy), rz],
            18 * f + 8 + 5 * (dy > 0) + piece,
            device(0, dy, 0),
        )

    plane = [[plane_copy(f, n) for n in range(8)] for f in range(3)]
    slab = [[[slab_copy(f, dy, p) for p in range(5)] for dy in (-1, 1)] for f in range(3)]

    def start_own(f):
        for dy in range(2):
            slab[f][dy][0].start()
        for copy in plane[f]:
            copy.start()

    def forward(f):
        groups = (
            (1, [n for n, (dx, dz) in enumerate(PLANE) if dx == 1]),
            (2, [n for n, (dx, dz) in enumerate(PLANE) if dx == -1]),
            (3, [PLANE.index((0, 1))]),
            (4, [PLANE.index((0, -1))]),
        )
        for piece, needed in groups:
            for n in needed:
                plane[f][n].wait_recv()
            for dy in range(2):
                slab[f][dy][piece].start()

    def finish(f):
        for dy in range(2):
            for piece in range(5):
                slab[f][dy][piece].wait_recv()

    loads[0].wait()
    lane = lax.broadcasted_iota(jnp.int32, (32, 128), 1)

    def mask_x(x, carry):
        for y in range(4):
            for z in range(4):
                live = (lane < counts[x, y, z]).astype(F32).astype(BF)
                ext[x + 1, y + 1, z + 1] = raw[x, y, z] * live
        return carry

    lax.fori_loop(0, 4, mask_x, 0)
    pl.semaphore_wait(barrier, (nx - 1) + (ny * nz - 1) + 4)
    start_own(0)

    loads[1].wait()
    loads[2].wait()

    def leaf_x(x, carry):
        for yp in range(2):
            for zp in range(2):
                box = ext[x + 1, pl.ds(2 * yp + 1, 2), pl.ds(2 * zp + 1, 2)]
                value = dot(basis[...], box.reshape(128, 128), 1, 1)
                mom[0, x + 2, yp + 1, zp + 1] = value.astype(BF)
        return carry

    lax.fori_loop(0, 4, leaf_x, 0)
    start_own(1)

    for cx in range(2):
        acc = jnp.zeros((48, 128), F32)
        for i in range(2):
            quads = [mom[0, 2 * cx + i + 2, cy + 1, cz + 1] for cy in range(2) for cz in range(2)]
            for jl in range(4):
                kids = jnp.concatenate([q[:, 32 * jl : 32 * jl + 32] for q in quads], axis=1)
                acc = acc + dot(transfer[4 * i + jl], kids)
        one[0, cx + 2, 1, 1] = acc.astype(BF)
    start_own(2)

    acc = jnp.zeros((48, 32), F32)
    for i in range(2):
        own = one[0, i + 2, 1, 1]
        for jl in range(4):
            acc = acc + dot(transfer[4 * i + jl], own[:, 32 * jl : 32 * jl + 32])
    gathered[0] = pack(acc).astype(BF)

    def gather_copy(d):
        return pltpu.make_async_remote_copy(
            src_ref=gathered.at[0],
            dst_ref=gathered.at[d],
            send_sem=g_send.at[d],
            recv_sem=g_recv.at[d],
            device_id=device(d, 0, 0),
            device_id_type=MESH,
        )

    def gather_start(d, carry):
        gather_copy(d).start()
        return carry

    lax.fori_loop(1, nx, gather_start, 0)

    codes = [9 * near_off[0, s] + 3 * near_off[1, s] + near_off[2, s] + 13 for s in range(27)]
    for s in range(27):
        inverse[27 + s] = codes[s]

    def invert(c, carry):
        found = jnp.int32(0)
        for s in range(27):
            found = jnp.where(inverse[27 + s] == c, jnp.int32(s), found)
        inverse[c] = found
        return carry

    lax.fori_loop(0, 27, invert, 0)
    for level in range(2):
        for e in range(32):
            ox = far_off[0, level, e] + 2
            ay = far_off[1, level, e] + 2
            az = far_off[2, level, e] + 2
            half_y, half_z = lax.shift_right_logical(ay, 1), lax.shift_right_logical(az, 1)
            kind = 2 * (ay - 2 * half_y) + (az - 2 * half_z)
            if level == 0:
                base[e] = ((kind * 8 + ox) * 4 + half_y) * 4 + half_z
            else:
                base[32 + e] = ((kind * 6 + ox) * 3 + half_y) * 3 + half_z

    loads[3].wait()

    def build(c, carry):
        taps = [blocks[inverse[3 * c + t]].T for t in range(3)]
        zero = jnp.zeros((128, 128), BF)
        toep[c, 0:128, 0:128] = taps[0]
        toep[c, 0:128, 128:256] = zero
        toep[c, 128:256, 0:128] = taps[1]
        toep[c, 128:256, 128:256] = taps[0]
        toep[c, 256:384, 0:128] = taps[2]
        toep[c, 256:384, 128:256] = taps[1]
        toep[c, 384:512, 0:128] = zero
        toep[c, 384:512, 128:256] = taps[2]
        return carry

    lax.fori_loop(0, 9, build, 0)

    loads[5].wait()
    for level in range(2):
        for e in range(32):
            packed[level, :, 48 * e : 48 * e + 48] = coupling[level, e]

    loads[4].wait()

    def gather_wait(d, carry):
        gather_copy(d).wait_recv()
        return carry

    lax.fori_loop(1, nx, gather_wait, 0)

    def partial(dy, carry):
        acc = jnp.zeros((192, 32), F32)
        for d in range(nx):
            mats = coarse[(nx - d) % nx, dy].reshape(192, 48)
            acc = acc + dot(mats, unpack(gathered[d]))
        for dz in range(4):
            part_out[4 * dy + dz] = pack(acc[48 * dz : 48 * dz + 48])
        return carry

    lax.fori_loop(0, 4, partial, 0)

    def part_copy(d):
        return pltpu.make_async_remote_copy(
            src_ref=part_out.at[d],
            dst_ref=part_in.at[d],
            send_sem=p_send.at[d],
            recv_sem=p_recv.at[d],
            device_id=device(0, -(d // nz), -(d % nz)),
            device_id_type=MESH,
        )

    def part_start(d, carry):
        part_copy(d).start()
        return carry

    lax.fori_loop(1, ny * nz, part_start, 0)

    for f in range(3):
        forward(f)

    def lhs(x, ys, count):
        parts = []
        for step in range(3):
            rows = [
                jnp.concatenate([ext[x + step, pl.ds(ys, count), 2 * zp + j] for j in range(4)], axis=2)
                for zp in range(2)
            ]
            stacked = jnp.stack(rows, axis=1)
            parts.append(stacked.reshape(count * 64, 512))
        return parts

    def near_x(x, carry):
        for dy, ys, count, row in ((1, 1, 4, 0), (0, 1, 3, 1), (2, 2, 3, 0)):
            acc = sum(dot(v, toep[3 * step + dy]) for step, v in enumerate(lhs(x, ys, count)))
            acc = acc.reshape(count, 64, 256)
            if dy == 1:
                near[x] = acc
            else:
                near[x, row : row + 3] += acc
        return carry

    lax.fori_loop(0, 4, near_x, 0)

    finish(2)

    def shifts(buf, xs, side, x):
        def ahead_z(a, b):
            return jnp.concatenate([a[:, 32:64], b[:, 0:32], a[:, 96:128], b[:, 64:96]], axis=1)

        def ahead_y(a, b):
            return jnp.concatenate([a[:, 64:128], b[:, 0:64]], axis=1)

        for yp in range(side):
            for zp in range(side - 1):
                buf[1, x, yp, zp] = ahead_z(buf[0, x, yp, zp], buf[0, x, yp, zp + 1])
        for yp in range(side - 1):
            for zp in range(side):
                buf[2, x, yp, zp] = ahead_y(buf[0, x, yp, zp], buf[0, x, yp + 1, zp])
        for yp in range(side - 1):
            for zp in range(side - 1):
                buf[3, x, yp, zp] = ahead_y(buf[1, x, yp, zp], buf[1, x, yp + 1, zp])

    def shift_one(x, carry):
        shifts(one, 6, 3, x)
        return carry

    lax.fori_loop(0, 6, shift_one, 0)
    flat_one = one.reshape(4 * 6 * 3 * 3, 48, 128)
    sides = []
    for cx in range(2):
        sides.append(
            jnp.concatenate([flat_one[base[32 + e] + cx * 9] for e in range(32)], axis=0)
        )
    local_one = dot(packed[1], jnp.concatenate(sides, axis=1))

    def part_wait(d, carry):
        part_copy(d).wait_recv()
        return carry

    lax.fori_loop(1, ny * nz, part_wait, 0)
    total = part_out[0]
    for d in range(1, ny * nz):
        total = total + part_in[d]
    local_two = unpack(total).astype(BF)
    for cx in range(2):
        spread = jnp.concatenate(
            [dot(transfer[4 * cx + jl], local_two, 0, 0) for jl in range(4)], axis=1
        )
        total_one = (local_one[:, 128 * cx : 128 * cx + 128] + spread).astype(BF)
        for i in range(2):
            pieces = [dot(transfer[4 * i + jl], total_one, 0, 0) for jl in range(4)]
            for quad in range(4):
                down[2 * cx + i, quad] = jnp.concatenate(
                    [p[:, 32 * quad : 32 * quad + 32] for p in pieces], axis=1
                )

    finish(0)
    for dy, ext_y, y in ((0, 0, 0), (2, 5, 3)):
        acc = jnp.zeros((256, 256), F32)
        for step in range(3):
            rows = [
                jnp.concatenate([ext[pl.ds(step, 4), ext_y, 2 * zp + j] for j in range(4)], axis=2)
                for zp in range(2)
            ]
            acc = acc + dot(jnp.stack(rows, axis=1).reshape(256, 512), toep[3 * step + dy])
        near[:, y] += acc.reshape(4, 64, 256)

    finish(1)

    def shift_mom(x, carry):
        shifts(mom, 8, 4, x)
        return carry

    lax.fori_loop(0, 8, shift_mom, 0)
    flat_mom = mom.reshape(4 * 8 * 4 * 4, 48, 128)

    def leaf_level(t, carry):
        x, yp = t // 2, t % 2
        offset = x * 16 + yp * 4
        sides = [
            jnp.concatenate([flat_mom[base[e] + (offset + zp)] for e in range(32)], axis=0)
            for zp in range(2)
        ]
        local = dot(packed[0], jnp.concatenate(sides, axis=1))
        for zp in range(2):
            total = (local[:, 128 * zp : 128 * zp + 128] + down[x, 2 * yp + zp]).astype(BF)
            far = dot(total, basis[...], 0, 0)
            for y2 in range(2):
                for z2 in range(2):
                    y, z = 2 * yp + y2, 2 * zp + z2
                    live = lane < counts[x, y, z]
                    row = 64 * y2 + 32 * z2
                    value = near[x, y, 32 * zp : 32 * zp + 32, 128 * z2 : 128 * z2 + 128]
                    out[x, y, z] = jnp.where(live, value + far[row : row + 32], 0.0)
        return carry

    lax.fori_loop(0, 8, leaf_level, 0)

    for f in range(3):
        for copy in plane[f]:
            copy.wait_send()
        for dy in range(2):
            for copy in slab[f][dy]:
                copy.wait_send()

    def sent_line(d, carry):
        gather_copy(d).wait_send()
        return carry

    lax.fori_loop(1, nx, sent_line, 0)

    def sent_plane(d, carry):
        part_copy(d).wait_send()
        return carry

    lax.fori_loop(1, ny * nz, sent_plane, 0)


def body(
    sizes,
    charges,
    counts,
    near_offsets,
    near_blocks,
    leaf_basis,
    transfer,
    far_offsets,
    coupling,
    coarse_coupling,
):
    smem = pl.BlockSpec(memory_space=pltpu.SMEM)
    hbm = pl.BlockSpec(memory_space=pl.ANY)
    vmem = pl.BlockSpec(memory_space=pltpu.VMEM)
    dma = pltpu.SemaphoreType.DMA
    nx, ny, nz = sizes
    return pl.pallas_call(
        functools.partial(kernel, sizes),
        out_shape=jax.ShapeDtypeStruct((4, 4, 4, 32, 128), F32),
        in_specs=[smem] * 3 + [hbm] * 6,
        out_specs=vmem,
        scratch_shapes=[
            pltpu.VMEM((6, 6, 6, 32, 128), BF),
            pltpu.VMEM((4, 8, 4, 4, 48, 128), BF),
            pltpu.VMEM((4, 6, 3, 3, 48, 128), BF),
            pltpu.VMEM((4, 4, 4, 32, 128), BF),
            pltpu.VMEM((27, 128, 128), BF),
            pltpu.VMEM((48, 128), BF),
            pltpu.VMEM((8, 48, 48), BF),
            pltpu.VMEM((2, 32, 48, 48), BF),
            pltpu.VMEM((16, 4, 4, 48, 48), BF),
            pltpu.VMEM((9, 512, 256), BF),
            pltpu.VMEM((2, 48, 1536), BF),
            pltpu.VMEM((4, 4, 64, 256), F32),
            pltpu.VMEM((nx, 16, 128), BF),
            pltpu.VMEM((ny * nz, 16, 128), F32),
            pltpu.VMEM((ny * nz, 16, 128), F32),
            pltpu.VMEM((4, 4, 48, 128), F32),
            pltpu.SMEM((64,), jnp.int32),
            pltpu.SMEM((64,), jnp.int32),
            dma((6,)),
            dma((54,)),
            dma((54,)),
            dma((nx,)),
            dma((nx,)),
            dma((ny * nz,)),
            dma((ny * nz,)),
        ],
        compiler_params=pltpu.CompilerParams(
            collective_id=0, has_side_effects=True, vmem_limit_bytes=60 * 1024 * 1024
        ),
    )(
        counts,
        near_offsets.T,
        far_offsets.transpose(2, 0, 1),
        charges,
        near_blocks,
        leaf_basis,
        transfer,
        coupling,
        coarse_coupling,
    )


def solution(mesh):
    sizes = (mesh.shape["gx"], mesh.shape["gy"], mesh.shape["gz"])
    spread = P("gx", "gy", "gz", None, None)
    in_specs = (spread, P("gx", "gy", "gz"), P(), P(), P(), P(), P(), P(), P())
    return jax.shard_map(
        functools.partial(body, sizes),
        mesh=mesh,
        in_specs=in_specs,
        out_specs=spread,
        check_vma=False,
    )
```

```python
import functools

import jax
import jax.numpy as jnp
from jax import lax
from jax.experimental import pallas as pl
from jax.experimental.pallas import tpu as pltpu
from jax.sharding import PartitionSpec as P

MESH = pl.DeviceIdType.MESH
BF = jnp.bfloat16
F32 = jnp.float32

FIELDS = (
    ((1, 5, 1), (1, 5, 1), (1, 5, 1)),
    ((2, 6, 2), (1, 3, 1), (1, 3, 1)),
    ((2, 4, 2), (1, 2, 1), (1, 2, 1)),
)
SEMS = 18


def own(axis):
    return pl.ds(axis[0], axis[1] - axis[0])


def source(axis, step):
    low, high, width = axis
    return pl.ds(high - width, width) if step > 0 else pl.ds(low, width)


def target(axis, step):
    low, high, width = axis
    return pl.ds(low - width, width) if step > 0 else pl.ds(high, width)


def dot(a, b, contract_a=1, contract_b=0):
    return lax.dot_general(
        a, b, (((contract_a,), (contract_b,)), ((), ())), preferred_element_type=F32
    )


def pack(value):
    zero = jnp.zeros((16, 32), value.dtype)
    return jnp.concatenate([value[0:16], value[16:32], value[32:48], zero], axis=1)


def unpack(value):
    return jnp.concatenate([value[:, 0:32], value[:, 32:64], value[:, 64:96]], axis=0)


def kernel(
    sizes,
    counts,
    near_off,
    far_off,
    charges,
    near_blocks,
    basis_hbm,
    transfer_hbm,
    coupling_hbm,
    coarse_hbm,
    out,
    ext,
    mom,
    one,
    raw,
    blocks,
    basis,
    transfer,
    coupling,
    coarse,
    toep,
    packed,
    near,
    result,
    gathered,
    part_out,
    part_in,
    down,
    inverse,
    base,
    in_sem,
    out_sem,
    send_sem,
    recv_sem,
    g_send,
    g_recv,
    p_send,
    p_recv,
):
    nx, ny, nz = sizes
    mx, my, mz = lax.axis_index("gx"), lax.axis_index("gy"), lax.axis_index("gz")

    odd = lax.rem(mz, 2)
    flip = 2 * odd - 1

    def device(dx, dy, dz):
        return {
            "gx": lax.rem(mx + (dx + nx), nx),
            "gy": lax.rem(my + (dy + ny), ny),
            "gz": lax.rem(mz + (dz + nz), nz),
        }

    loads = [
        pltpu.make_async_copy(src, dst, in_sem.at[i])
        for i, (src, dst) in enumerate(
            (
                (charges, raw),
                (basis_hbm, basis),
                (transfer_hbm, transfer),
                (near_blocks, blocks),
                (coarse_hbm, coarse),
                (coupling_hbm, coupling),
            )
        )
    ]
    for copy in loads:
        copy.start()

    barrier = pltpu.get_barrier_semaphore()
    for dx in (-1, 1):
        pl.semaphore_signal(barrier, inc=1, device_id=device(dx, 0, flip), device_id_type=MESH)

    def greet_line(d, carry):
        pl.semaphore_signal(barrier, inc=1, device_id=device(d, 0, 0), device_id_type=MESH)
        return carry

    lax.fori_loop(1, nx, greet_line, 0)

    def greet_plane(d, carry):
        pl.semaphore_signal(
            barrier, inc=1, device_id=device(0, d // nz, d % nz), device_id_type=MESH
        )
        return carry

    lax.fori_loop(1, ny * nz, greet_plane, 0)

    bufs = (ext, mom.at[0], one.at[0])

    def remote(f, sem, to, src, dst):
        return pltpu.make_async_remote_copy(
            src_ref=bufs[f].at[src],
            dst_ref=bufs[f].at[dst],
            send_sem=send_sem.at[SEMS * f + sem],
            recv_sem=recv_sem.at[SEMS * f + sem],
            device_id=to,
            device_id_type=MESH,
        )

    def copies(f):
        ax, ay, az = FIELDS[f]
        low, high, width = az
        span = high - low
        wide = span + width
        outer_src = pl.ds(low + odd * (span - width), width)
        inner_src = pl.ds(high - width - odd * (span - width), width)
        outer_dst = pl.ds(low - width + odd * wide, width)
        inner_dst = pl.ds(high - odd * wide, width)
        own_outer = pl.ds(low - width + odd * width, wide)
        plane = {}
        for dx in (-1, 0, 1):
            rx = (source(ax, dx), target(ax, dx)) if dx else (own(ax), own(ax))
            if dx:
                plane[dx, 0] = remote(
                    f, (dx + 1) // 2, device(dx, 0, 0),
                    (rx[0], own(ay), own(az)), (rx[1], own(ay), own(az)),
                )
            plane[dx, 1] = remote(
                f, 3 + dx, device(dx, 0, flip),
                (rx[0], own(ay), outer_src), (rx[1], own(ay), inner_dst),
            )
        slab = {}
        regions = {
            "own": (own(ax), own(az)),
            "low": (target(ax, 1), own_outer),
            "high": (target(ax, -1), own_outer),
            "outer": (own(ax), outer_dst),
        }
        for j, dy in enumerate((-1, 1)):
            for i, (name, (rx, rz)) in enumerate(regions.items()):
                slab[dy, name] = remote(
                    f, 5 + 4 * j + i, device(0, dy, 0),
                    (rx, source(ay, dy), rz), (rx, target(ay, dy), rz),
                )
        side = {}
        full = pl.ds(0, ax[1] + ax[2])
        regions = {
            "own": (own(ax), own(ay)),
            "low": (target(ax, 1), own(ay)),
            "high": (target(ax, -1), own(ay)),
            1: (full, target(ay, 1)),
            -1: (full, target(ay, -1)),
        }
        for i, (name, (rx, ry)) in enumerate(regions.items()):
            side[name] = remote(
                f, 13 + i, device(0, 0, -flip), (rx, ry, inner_src), (rx, ry, outer_dst)
            )
        return plane, slab, side

    planes, slabs, sides = zip(*[copies(f) for f in range(3)])

    def start_slab(f):
        for dy in (-1, 1):
            slabs[f][dy, "own"].start()

    def start_plane(f):
        sides[f]["own"].start()
        for copy in planes[f].values():
            copy.start()

    def forward(f):
        for name, dx in (("low", 1), ("high", -1)):
            planes[f][dx, 0].wait_recv()
            sides[f][name].start()
            planes[f][dx, 1].wait_recv()
            for dy in (-1, 1):
                slabs[f][dy, name].start()
        planes[f][0, 1].wait_recv()
        for dy in (-1, 1):
            slabs[f][dy, "outer"].start()

    def hand_over(f):
        for dy in (-1, 1):
            for name in ("own", "low", "high"):
                slabs[f][dy, name].wait_recv()
            sides[f][dy].start()

    def finish(f):
        for dy in (-1, 1):
            slabs[f][dy, "outer"].wait_recv()
        for name, copy in sides[f].items():
            if f != 0 or name in (-1, 1):
                copy.wait_recv()

    loads[0].wait()
    lane = lax.broadcasted_iota(jnp.int32, (32, 128), 1)

    def mask_x(x, carry):
        for y in range(4):
            for z in range(4):
                live = (lane < counts[x, y, z]).astype(F32).astype(BF)
                ext[x + 1, y + 1, z + 1] = raw[x, y, z] * live
        return carry

    lax.fori_loop(0, 4, mask_x, 0)

    loads[1].wait()
    loads[2].wait()

    def leaf_x(x, carry):
        for yp in range(2):
            for zp in range(2):
                box = ext[x + 1, pl.ds(2 * yp + 1, 2), pl.ds(2 * zp + 1, 2)]
                value = dot(basis[...], box.reshape(128, 128), 1, 1)
                mom[0, x + 2, yp + 1, zp + 1] = value.astype(BF)
        return carry

    lax.fori_loop(0, 4, leaf_x, 0)

    for cx in range(2):
        acc = jnp.zeros((48, 128), F32)
        for i in range(2):
            quads = [mom[0, 2 * cx + i + 2, cy + 1, cz + 1] for cy in range(2) for cz in range(2)]
            for jl in range(4):
                kids = jnp.concatenate([q[:, 32 * jl : 32 * jl + 32] for q in quads], axis=1)
                acc = acc + dot(transfer[4 * i + jl], kids)
        one[0, cx + 2, 1, 1] = acc.astype(BF)

    acc = jnp.zeros((48, 32), F32)
    for i in range(2):
        box = one[0, i + 2, 1, 1]
        for jl in range(4):
            acc = acc + dot(transfer[4 * i + jl], box[:, 32 * jl : 32 * jl + 32])
    gathered[0] = pack(acc).astype(BF)

    def gather_copy(d):
        return pltpu.make_async_remote_copy(
            src_ref=gathered.at[0],
            dst_ref=gathered.at[d],
            send_sem=g_send.at[d],
            recv_sem=g_recv.at[d],
            device_id=device(d, 0, 0),
            device_id_type=MESH,
        )

    def gather_start(d, carry):
        gather_copy(d).start()
        return carry

    pl.semaphore_wait(barrier, (nx - 1) + (ny * nz - 1) + 2)
    lax.fori_loop(1, nx, gather_start, 0)
    start_plane(1)
    start_slab(1)
    start_plane(2)
    start_slab(2)
    start_plane(0)
    start_slab(0)

    codes = [9 * near_off[0, s] + 3 * near_off[1, s] + near_off[2, s] + 13 for s in range(27)]
    for s in range(27):
        inverse[27 + s] = codes[s]

    def invert(c, carry):
        found = jnp.int32(0)
        for s in range(27):
            found = jnp.where(inverse[27 + s] == c, jnp.int32(s), found)
        inverse[c] = found
        return carry

    lax.fori_loop(0, 27, invert, 0)
    for level in range(2):
        for e in range(32):
            ox = far_off[0, level, e] + 2
            ay = far_off[1, level, e] + 2
            az = far_off[2, level, e] + 2
            half_y, half_z = lax.shift_right_logical(ay, 1), lax.shift_right_logical(az, 1)
            kind = 2 * (ay - 2 * half_y) + (az - 2 * half_z)
            if level == 0:
                base[e] = ((kind * 8 + ox) * 4 + half_y) * 4 + half_z
            else:
                base[32 + e] = ((kind * 6 + ox) * 3 + half_y) * 3 + half_z

    loads[3].wait()

    def build(c, carry):
        taps = [blocks[inverse[3 * c + t]].T for t in range(3)]
        zero = jnp.zeros((128, 128), BF)
        toep[c, 0:128, 0:128] = taps[0]
        toep[c, 0:128, 128:256] = zero
        toep[c, 128:256, 0:128] = taps[1]
        toep[c, 128:256, 128:256] = taps[0]
        toep[c, 256:384, 0:128] = taps[2]
        toep[c, 256:384, 128:256] = taps[1]
        toep[c, 384:512, 0:128] = zero
        toep[c, 384:512, 128:256] = taps[2]
        return carry

    lax.fori_loop(0, 9, build, 0)

    loads[5].wait()
    for level in range(2):
        for e in range(32):
            packed[level, :, 48 * e : 48 * e + 48] = coupling[level, e]

    loads[4].wait()

    def gather_wait(d, carry):
        gather_copy(d).wait_recv()
        return carry

    lax.fori_loop(1, nx, gather_wait, 0)

    def partial(dy, carry):
        acc = jnp.zeros((192, 32), F32)
        for d in range(nx):
            mats = coarse[(nx - d) % nx, dy].reshape(192, 48)
            acc = acc + dot(mats, unpack(gathered[d]))
        for dz in range(4):
            part_out[4 * dy + dz] = pack(acc[48 * dz : 48 * dz + 48])
        return carry

    lax.fori_loop(0, 4, partial, 0)

    def part_copy(d):
        return pltpu.make_async_remote_copy(
            src_ref=part_out.at[d],
            dst_ref=part_in.at[d],
            send_sem=p_send.at[d],
            recv_sem=p_recv.at[d],
            device_id=device(0, -(d // nz), -(d % nz)),
            device_id_type=MESH,
        )

    def part_start(d, carry):
        part_copy(d).start()
        return carry

    lax.fori_loop(1, ny * nz, part_start, 0)

    forward(1)
    forward(2)

    group = lax.broadcasted_iota(jnp.int32, (48, 128), 1)
    even_z = (group % 64) < 32
    first_y = group < 64

    def shifts(buf, side, x):
        def ahead_y(a, b):
            return jnp.where(first_y, pltpu.roll(a, 64, 1), pltpu.roll(b, 64, 1))

        plain = [[buf[0, x, yp, zp] for zp in range(side)] for yp in range(side)]
        moved = []
        for yp in range(side):
            down_z = [pltpu.roll(v, 96, 1) for v in plain[yp][:-1]]
            up_z = [pltpu.roll(v, 32, 1) for v in plain[yp][1:]]
            moved.append([jnp.where(even_z, a, b) for a, b in zip(down_z, up_z)])
            for zp in range(side - 1):
                buf[1, x, yp, zp] = moved[yp][zp]
        for kind, rows in ((2, plain), (3, moved)):
            turned = [[pltpu.roll(v, 64, 1) for v in row] for row in rows]
            for yp in range(side - 1):
                for zp in range(len(rows[0])):
                    buf[kind, x, yp, zp] = jnp.where(
                        first_y, turned[yp][zp], turned[yp + 1][zp]
                    )

    hand_over(1)
    finish(1)

    def shift_mom(x, carry):
        shifts(mom, 4, x)
        return carry

    lax.fori_loop(0, 8, shift_mom, 0)
    flat_mom = mom.reshape(4 * 8 * 4 * 4, 48, 128)

    def leaf_list(t, carry):
        x, yp = t // 2, t % 2
        offset = x * 16 + yp * 4
        windows = [
            jnp.concatenate([flat_mom[base[e] + (offset + zp)] for e in range(32)], axis=0)
            for zp in range(2)
        ]
        local = dot(packed[0], jnp.concatenate(windows, axis=1))
        for zp in range(2):
            down[x, 2 * yp + zp] = local[:, 128 * zp : 128 * zp + 128]
        return carry

    lax.fori_loop(0, 4, leaf_list, 0)
    hand_over(2)
    forward(0)
    lax.fori_loop(4, 8, leaf_list, 0)

    finish(2)

    def shift_one(x, carry):
        shifts(one, 3, x)
        return carry

    lax.fori_loop(0, 6, shift_one, 0)
    flat_one = one.reshape(4 * 6 * 3 * 3, 48, 128)
    windows = [
        jnp.concatenate([flat_one[base[32 + e] + cx * 9] for e in range(32)], axis=0)
        for cx in range(2)
    ]
    local_one = dot(packed[1], jnp.concatenate(windows, axis=1))

    def part_wait(d, carry):
        part_copy(d).wait_recv()
        return carry

    lax.fori_loop(1, ny * nz, part_wait, 0)
    total = part_out[0]
    for d in range(1, ny * nz):
        total = total + part_in[d]
    local_two = unpack(total).astype(BF)
    for cx in range(2):
        spread = jnp.concatenate(
            [dot(transfer[4 * cx + jl], local_two, 0, 0) for jl in range(4)], axis=1
        )
        total_one = (local_one[:, 128 * cx : 128 * cx + 128] + spread).astype(BF)
        for i in range(2):
            pieces = [dot(transfer[4 * i + jl], total_one, 0, 0) for jl in range(4)]
            for quad in range(4):
                down[2 * cx + i, quad] += jnp.concatenate(
                    [p[:, 32 * quad : 32 * quad + 32] for p in pieces], axis=1
                )

    def far_x(x, carry):
        for yp in range(2):
            for zp in range(2):
                far = dot(down[x, 2 * yp + zp].astype(BF), basis[...], 0, 0)
                for y2 in range(2):
                    for z2 in range(2):
                        row = 64 * y2 + 32 * z2
                        near[
                            x, 2 * yp + y2, 32 * zp : 32 * zp + 32, 128 * z2 : 128 * z2 + 128
                        ] = far[row : row + 32]
        return carry

    lax.fori_loop(0, 4, far_x, 0)

    for name in ("own", "low", "high"):
        sides[0][name].wait_recv()

    def lhs(x, ys, count):
        parts = []
        for step in range(3):
            rows = [
                jnp.concatenate([ext[x + step, pl.ds(ys, count), 2 * zp + j] for j in range(4)], axis=2)
                for zp in range(2)
            ]
            stacked = jnp.stack(rows, axis=1)
            parts.append(stacked.reshape(count * 64, 512))
        return parts

    def near_x(x, carry):
        for dy, ys, count, row in ((1, 1, 4, 0), (0, 1, 3, 1), (2, 2, 3, 0)):
            acc = sum(dot(v, toep[3 * step + dy]) for step, v in enumerate(lhs(x, ys, count)))
            near[x, row : row + count] += acc.reshape(count, 64, 256)
        return carry

    lax.fori_loop(0, 4, near_x, 0)
    hand_over(0)

    def write(y):
        for x in range(4):
            for z in range(4):
                zp, z2 = z // 2, z % 2
                value = near[x, y, 32 * zp : 32 * zp + 32, 128 * z2 : 128 * z2 + 128]
                result[x, y, z] = jnp.where(lane < counts[x, y, z], value, 0.0)
        copy = pltpu.make_async_copy(result.at[:, y], out.at[:, y], out_sem.at[y])
        copy.start()
        return copy

    stores = [write(1), write(2)]

    finish(0)
    for dy, ext_y, y in ((0, 0, 0), (2, 5, 3)):
        acc = jnp.zeros((256, 256), F32)
        for step in range(3):
            rows = [
                jnp.concatenate([ext[pl.ds(step, 4), ext_y, 2 * zp + j] for j in range(4)], axis=2)
                for zp in range(2)
            ]
            acc = acc + dot(jnp.stack(rows, axis=1).reshape(256, 512), toep[3 * step + dy])
        near[:, y] += acc.reshape(4, 64, 256)
        stores.append(write(y))
    for copy in stores:
        copy.wait()

    for f in range(3):
        for group in (planes[f], slabs[f], sides[f]):
            for copy in group.values():
                copy.wait_send()

    def sent_line(d, carry):
        gather_copy(d).wait_send()
        return carry

    lax.fori_loop(1, nx, sent_line, 0)

    def sent_plane(d, carry):
        part_copy(d).wait_send()
        return carry

    lax.fori_loop(1, ny * nz, sent_plane, 0)


def body(
    sizes,
    charges,
    counts,
    near_offsets,
    near_blocks,
    leaf_basis,
    transfer,
    far_offsets,
    coupling,
    coarse_coupling,
):
    smem = pl.BlockSpec(memory_space=pltpu.SMEM)
    hbm = pl.BlockSpec(memory_space=pl.ANY)
    dma = pltpu.SemaphoreType.DMA
    nx, ny, nz = sizes
    return pl.pallas_call(
        functools.partial(kernel, sizes),
        out_shape=jax.ShapeDtypeStruct((4, 4, 4, 32, 128), F32),
        in_specs=[smem] * 3 + [hbm] * 6,
        out_specs=hbm,
        scratch_shapes=[
            pltpu.VMEM((6, 6, 6, 32, 128), BF),
            pltpu.VMEM((4, 8, 4, 4, 48, 128), BF),
            pltpu.VMEM((4, 6, 3, 3, 48, 128), BF),
            pltpu.VMEM((4, 4, 4, 32, 128), BF),
            pltpu.VMEM((27, 128, 128), BF),
            pltpu.VMEM((48, 128), BF),
            pltpu.VMEM((8, 48, 48), BF),
            pltpu.VMEM((2, 32, 48, 48), BF),
            pltpu.VMEM((16, 4, 4, 48, 48), BF),
            pltpu.VMEM((9, 512, 256), BF),
            pltpu.VMEM((2, 48, 1536), BF),
            pltpu.VMEM((4, 4, 64, 256), F32),
            pltpu.VMEM((4, 4, 4, 32, 128), F32),
            pltpu.VMEM((nx, 16, 128), BF),
            pltpu.VMEM((ny * nz, 16, 128), F32),
            pltpu.VMEM((ny * nz, 16, 128), F32),
            pltpu.VMEM((4, 4, 48, 128), F32),
            pltpu.SMEM((64,), jnp.int32),
            pltpu.SMEM((64,), jnp.int32),
            dma((6,)),
            dma((4,)),
            dma((3 * SEMS,)),
            dma((3 * SEMS,)),
            dma((nx,)),
            dma((nx,)),
            dma((ny * nz,)),
            dma((ny * nz,)),
        ],
        compiler_params=pltpu.CompilerParams(
            collective_id=0, has_side_effects=True, vmem_limit_bytes=60 * 1024 * 1024
        ),
    )(
        counts,
        near_offsets.T,
        far_offsets.transpose(2, 0, 1),
        charges,
        near_blocks,
        leaf_basis,
        transfer,
        coupling,
        coarse_coupling,
    )


def solution(mesh):
    sizes = (mesh.shape["gx"], mesh.shape["gy"], mesh.shape["gz"])
    spread = P("gx", "gy", "gz", None, None)
    in_specs = (spread, P("gx", "gy", "gz"), P(), P(), P(), P(), P(), P(), P())
    return jax.shard_map(
        functools.partial(body, sizes),
        mesh=mesh,
        in_specs=in_specs,
        out_specs=spread,
        check_vma=False,
    )
```

```python
import functools

import jax
import jax.numpy as jnp
from jax import lax
from jax.experimental import pallas as pl
from jax.experimental.pallas import tpu as pltpu
from jax.sharding import PartitionSpec as P

MESH = pl.DeviceIdType.MESH
BF = jnp.bfloat16
F32 = jnp.float32

FIELDS = (
    ((1, 5, 1), (1, 5, 1), (1, 5, 1)),
    ((2, 6, 2), (1, 3, 1), (1, 3, 1)),
    ((2, 4, 2), (1, 2, 1), (1, 2, 1)),
)
SEMS = 18


def own(axis):
    return pl.ds(axis[0], axis[1] - axis[0])


def source(axis, step):
    low, high, width = axis
    return pl.ds(high - width, width) if step > 0 else pl.ds(low, width)


def target(axis, step):
    low, high, width = axis
    return pl.ds(low - width, width) if step > 0 else pl.ds(high, width)


def dot(a, b, contract_a=1, contract_b=0):
    return lax.dot_general(
        a, b, (((contract_a,), (contract_b,)), ((), ())), preferred_element_type=F32
    )


def pack(value):
    zero = jnp.zeros((16, 32), value.dtype)
    return jnp.concatenate([value[0:16], value[16:32], value[32:48], zero], axis=1)


def unpack(value):
    return jnp.concatenate([value[:, 0:32], value[:, 32:64], value[:, 64:96]], axis=0)


def kernel(
    sizes,
    counts,
    near_off,
    far_off,
    charges,
    near_blocks,
    basis_hbm,
    transfer_hbm,
    coupling_hbm,
    coarse_hbm,
    out,
    ext,
    mom,
    one,
    raw,
    blocks,
    basis,
    transfer,
    coupling,
    coarse,
    toep,
    packed,
    near,
    result,
    gathered,
    part_out,
    part_in,
    down,
    inverse,
    base,
    in_sem,
    out_sem,
    send_sem,
    recv_sem,
    g_send,
    g_recv,
    p_send,
    p_recv,
):
    nx, ny, nz = sizes
    mx, my, mz = lax.axis_index("gx"), lax.axis_index("gy"), lax.axis_index("gz")

    odd = lax.rem(mz, 2)
    flip = 2 * odd - 1

    def device(dx, dy, dz):
        return {
            "gx": lax.rem(mx + (dx + nx), nx),
            "gy": lax.rem(my + (dy + ny), ny),
            "gz": lax.rem(mz + (dz + nz), nz),
        }

    loads = [
        pltpu.make_async_copy(src, dst, in_sem.at[i])
        for i, (src, dst) in enumerate(
            (
                (charges, raw),
                (basis_hbm, basis),
                (transfer_hbm, transfer),
                (near_blocks, blocks),
                (coarse_hbm, coarse),
                (coupling_hbm, coupling),
            )
        )
    ]
    for copy in loads:
        copy.start()

    barrier = pltpu.get_barrier_semaphore()
    for dx in (-1, 1):
        pl.semaphore_signal(barrier, inc=1, device_id=device(dx, 0, flip), device_id_type=MESH)

    def greet_line(d, carry):
        pl.semaphore_signal(barrier, inc=1, device_id=device(d, 0, 0), device_id_type=MESH)
        return carry

    lax.fori_loop(1, nx, greet_line, 0)

    def greet_plane(d, carry):
        pl.semaphore_signal(
            barrier, inc=1, device_id=device(0, d // nz, d % nz), device_id_type=MESH
        )
        return carry

    lax.fori_loop(1, ny * nz, greet_plane, 0)

    bufs = (ext, mom.at[0], one.at[0])

    def remote(f, sem, to, src, dst):
        return pltpu.make_async_remote_copy(
            src_ref=bufs[f].at[src],
            dst_ref=bufs[f].at[dst],
            send_sem=send_sem.at[SEMS * f + sem],
            recv_sem=recv_sem.at[SEMS * f + sem],
            device_id=to,
            device_id_type=MESH,
        )

    def copies(f):
        ax, ay, az = FIELDS[f]
        low, high, width = az
        span = high - low
        wide = span + width
        outer_src = pl.ds(low + odd * (span - width), width)
        inner_src = pl.ds(high - width - odd * (span - width), width)
        outer_dst = pl.ds(low - width + odd * wide, width)
        inner_dst = pl.ds(high - odd * wide, width)
        own_outer = pl.ds(low - width + odd * width, wide)
        plane = {}
        for dx in (-1, 0, 1):
            rx = (source(ax, dx), target(ax, dx)) if dx else (own(ax), own(ax))
            if dx:
                plane[dx, 0] = remote(
                    f, (dx + 1) // 2, device(dx, 0, 0),
                    (rx[0], own(ay), own(az)), (rx[1], own(ay), own(az)),
                )
            plane[dx, 1] = remote(
                f, 3 + dx, device(dx, 0, flip),
                (rx[0], own(ay), outer_src), (rx[1], own(ay), inner_dst),
            )
        slab = {}
        regions = {
            "own": (own(ax), own(az)),
            "low": (target(ax, 1), own_outer),
            "high": (target(ax, -1), own_outer),
            "outer": (own(ax), outer_dst),
        }
        for j, dy in enumerate((-1, 1)):
            for i, (name, (rx, rz)) in enumerate(regions.items()):
                slab[dy, name] = remote(
                    f, 5 + 4 * j + i, device(0, dy, 0),
                    (rx, source(ay, dy), rz), (rx, target(ay, dy), rz),
                )
        side = {}
        full = pl.ds(0, ax[1] + ax[2])
        regions = {
            "own": (own(ax), own(ay)),
            "low": (target(ax, 1), own(ay)),
            "high": (target(ax, -1), own(ay)),
            1: (full, target(ay, 1)),
            -1: (full, target(ay, -1)),
        }
        for i, (name, (rx, ry)) in enumerate(regions.items()):
            side[name] = remote(
                f, 13 + i, device(0, 0, -flip), (rx, ry, inner_src), (rx, ry, outer_dst)
            )
        return plane, slab, side

    planes, slabs, sides = zip(*[copies(f) for f in range(3)])

    def start_slab(f):
        for dy in (-1, 1):
            slabs[f][dy, "own"].start()

    def start_plane(f):
        sides[f]["own"].start()
        for step in ((-1, 0), (1, 0), (-1, 1), (1, 1), (0, 1)):
            planes[f][step].start()

    def forward(f):
        for name, dx in (("low", 1), ("high", -1)):
            planes[f][dx, 0].wait_recv()
            sides[f][name].start()
            planes[f][dx, 1].wait_recv()
            for dy in (-1, 1):
                slabs[f][dy, name].start()

    def forward_outer(f):
        planes[f][0, 1].wait_recv()
        for dy in (-1, 1):
            slabs[f][dy, "outer"].start()

    def middle(f):
        for name in ("own", "low", "high"):
            sides[f][name].wait_recv()

    def hand_over(f):
        for dy in (-1, 1):
            for name in ("own", "low", "high"):
                slabs[f][dy, name].wait_recv()
            sides[f][dy].start()

    def finish(f):
        for dy in (-1, 1):
            slabs[f][dy, "outer"].wait_recv()
            sides[f][dy].wait_recv()

    loads[0].wait()
    lane = lax.broadcasted_iota(jnp.int32, (32, 128), 1)

    def mask_x(x, carry):
        for y in range(4):
            for z in range(4):
                live = (lane < counts[x, y, z]).astype(F32).astype(BF)
                ext[x + 1, y + 1, z + 1] = raw[x, y, z] * live
        return carry

    lax.fori_loop(0, 4, mask_x, 0)

    loads[1].wait()
    loads[2].wait()

    def leaf_x(x, carry):
        for yp in range(2):
            for zp in range(2):
                box = ext[x + 1, pl.ds(2 * yp + 1, 2), pl.ds(2 * zp + 1, 2)]
                value = dot(basis[...], box.reshape(128, 128), 1, 1)
                mom[0, x + 2, yp + 1, zp + 1] = value.astype(BF)
        return carry

    lax.fori_loop(0, 4, leaf_x, 0)

    for cx in range(2):
        acc = jnp.zeros((48, 128), F32)
        for i in range(2):
            quads = [mom[0, 2 * cx + i + 2, cy + 1, cz + 1] for cy in range(2) for cz in range(2)]
            for jl in range(4):
                kids = jnp.concatenate([q[:, 32 * jl : 32 * jl + 32] for q in quads], axis=1)
                acc = acc + dot(transfer[4 * i + jl], kids)
        one[0, cx + 2, 1, 1] = acc.astype(BF)

    acc = jnp.zeros((48, 32), F32)
    for i in range(2):
        box = one[0, i + 2, 1, 1]
        for jl in range(4):
            acc = acc + dot(transfer[4 * i + jl], box[:, 32 * jl : 32 * jl + 32])
    gathered[0] = pack(acc).astype(BF)

    def gather_copy(d):
        return pltpu.make_async_remote_copy(
            src_ref=gathered.at[0],
            dst_ref=gathered.at[d],
            send_sem=g_send.at[d],
            recv_sem=g_recv.at[d],
            device_id=device(d, 0, 0),
            device_id_type=MESH,
        )

    def gather_start(d, carry):
        gather_copy(d).start()
        return carry

    pl.semaphore_wait(barrier, (nx - 1) + (ny * nz - 1) + 2)
    lax.fori_loop(1, nx, gather_start, 0)
    start_plane(1)
    start_slab(1)
    start_plane(2)
    start_slab(2)
    start_plane(0)
    start_slab(0)

    codes = [9 * near_off[0, s] + 3 * near_off[1, s] + near_off[2, s] + 13 for s in range(27)]
    for s in range(27):
        inverse[27 + s] = codes[s]

    def invert(c, carry):
        found = jnp.int32(0)
        for s in range(27):
            found = jnp.where(inverse[27 + s] == c, jnp.int32(s), found)
        inverse[c] = found
        return carry

    lax.fori_loop(0, 27, invert, 0)
    for level in range(2):
        for e in range(32):
            ox = far_off[0, level, e] + 2
            ay = far_off[1, level, e] + 2
            az = far_off[2, level, e] + 2
            half_y, half_z = lax.shift_right_logical(ay, 1), lax.shift_right_logical(az, 1)
            kind = 2 * (ay - 2 * half_y) + (az - 2 * half_z)
            if level == 0:
                base[e] = ((kind * 8 + ox) * 4 + half_y) * 4 + half_z
            else:
                base[32 + e] = ((kind * 6 + ox) * 3 + half_y) * 3 + half_z

    loads[3].wait()

    def build(c, carry):
        taps = [blocks[inverse[3 * c + t]].T for t in range(3)]
        zero = jnp.zeros((128, 128), BF)
        toep[c, 0:128, 0:128] = taps[0]
        toep[c, 0:128, 128:256] = zero
        toep[c, 128:256, 0:128] = taps[1]
        toep[c, 128:256, 128:256] = taps[0]
        toep[c, 256:384, 0:128] = taps[2]
        toep[c, 256:384, 128:256] = taps[1]
        toep[c, 384:512, 0:128] = zero
        toep[c, 384:512, 128:256] = taps[2]
        return carry

    lax.fori_loop(0, 9, build, 0)

    def boxes(xs, ys, zs):
        parts = [ext[xs, ys, z] for z in zs]
        rows = parts[0].shape[0] * parts[0].shape[1] * 32
        return jnp.concatenate(parts, axis=3).reshape(rows, 128 * len(zs))

    INNER = {1: (0, 4, 1), 0: (1, 3, 1), 2: (0, 3, 2)}
    for dx, (xo, count_x, xi) in INNER.items():
        for dy, (yo, count_y, yi) in INNER.items():
            for zp, zs, rows in ((0, (1, 2, 3), pl.ds(128, 384)), (1, (2, 3, 4), pl.ds(0, 384))):
                value = dot(
                    boxes(pl.ds(xi, count_x), pl.ds(yi, count_y), zs), toep[3 * dx + dy, rows]
                ).reshape(count_x, count_y, 32, 256)
                at = (pl.ds(xo, count_x), pl.ds(yo, count_y), pl.ds(32 * zp, 32))
                if (dx, dy) == (1, 1):
                    near[at] = value
                else:
                    near[at] += value

    loads[5].wait()
    for level in range(2):
        for e in range(32):
            packed[level, :, 48 * e : 48 * e + 48] = coupling[level, e]

    loads[4].wait()

    def gather_wait(d, carry):
        gather_copy(d).wait_recv()
        return carry

    lax.fori_loop(1, nx, gather_wait, 0)

    def partial(dy, carry):
        acc = jnp.zeros((192, 32), F32)
        for d in range(nx):
            mats = coarse[(nx - d) % nx, dy].reshape(192, 48)
            acc = acc + dot(mats, unpack(gathered[d]))
        for dz in range(4):
            part_out[4 * dy + dz] = pack(acc[48 * dz : 48 * dz + 48])
        return carry

    lax.fori_loop(0, 4, partial, 0)

    def part_copy(d):
        return pltpu.make_async_remote_copy(
            src_ref=part_out.at[d],
            dst_ref=part_in.at[d],
            send_sem=p_send.at[d],
            recv_sem=p_recv.at[d],
            device_id=device(0, -(d // nz), -(d % nz)),
            device_id_type=MESH,
        )

    def part_start(d, carry):
        part_copy(d).start()
        return carry

    lax.fori_loop(1, ny * nz, part_start, 0)

    group = lax.broadcasted_iota(jnp.int32, (48, 128), 1)
    even_z = (group % 64) < 32
    first_y = group < 64

    def ahead_y(a, b):
        return jnp.where(first_y, pltpu.roll(a, 64, 1), pltpu.roll(b, 64, 1))

    def shifts(buf, side, x, inner):
        middle_rows = range(1, side - 1)
        for yp in range(side):
            if (yp in middle_rows) == inner:
                line = [buf[0, x, yp, zp] for zp in range(side)]
                down_z = [pltpu.roll(v, 96, 1) for v in line[:-1]]
                up_z = [pltpu.roll(v, 32, 1) for v in line[1:]]
                for zp in range(side - 1):
                    buf[1, x, yp, zp] = jnp.where(even_z, down_z[zp], up_z[zp])
        for yp in range(side - 1):
            if (yp in middle_rows and yp + 1 in middle_rows) == inner:
                for zp in range(side):
                    buf[2, x, yp, zp] = ahead_y(buf[0, x, yp, zp], buf[0, x, yp + 1, zp])
                for zp in range(side - 1):
                    buf[3, x, yp, zp] = ahead_y(buf[1, x, yp, zp], buf[1, x, yp + 1, zp])

    def shift_all(buf, planes_x, side, inner):
        def step(x, carry):
            shifts(buf, side, x, inner)
            return carry

        lax.fori_loop(0, planes_x, step, 0, unroll=planes_x // 2)

    forward(1)
    forward_outer(1)
    forward(2)
    forward_outer(2)
    middle(1)
    shift_all(mom, 8, 4, True)
    middle(2)
    shift_all(one, 6, 3, True)
    hand_over(1)
    forward(0)
    finish(1)
    shift_all(mom, 8, 4, False)
    forward_outer(0)
    hand_over(2)
    flat_mom = mom.reshape(4 * 8 * 4 * 4, 48, 128)

    def leaf_list(t, carry):
        x, yp = t // 2, t % 2
        offset = x * 16 + yp * 4
        windows = [
            jnp.concatenate([flat_mom[base[e] + (offset + zp)] for e in range(32)], axis=0)
            for zp in range(2)
        ]
        local = dot(packed[0], jnp.concatenate(windows, axis=1))
        for zp in range(2):
            down[x, 2 * yp + zp] = local[:, 128 * zp : 128 * zp + 128]
        return carry

    lax.fori_loop(0, 4, leaf_list, 0, unroll=4)
    hand_over(0)
    lax.fori_loop(4, 8, leaf_list, 0, unroll=4)

    finish(2)

    shift_all(one, 6, 3, False)
    flat_one = one.reshape(4 * 6 * 3 * 3, 48, 128)
    windows = [
        jnp.concatenate([flat_one[base[32 + e] + cx * 9] for e in range(32)], axis=0)
        for cx in range(2)
    ]
    local_one = dot(packed[1], jnp.concatenate(windows, axis=1))

    def part_wait(d, carry):
        part_copy(d).wait_recv()
        return carry

    lax.fori_loop(1, ny * nz, part_wait, 0)
    total = part_out[0]
    for d in range(1, ny * nz):
        total = total + part_in[d]
    local_two = unpack(total).astype(BF)
    for cx in range(2):
        spread = jnp.concatenate(
            [dot(transfer[4 * cx + jl], local_two, 0, 0) for jl in range(4)], axis=1
        )
        total_one = (local_one[:, 128 * cx : 128 * cx + 128] + spread).astype(BF)
        for i in range(2):
            pieces = [dot(transfer[4 * i + jl], total_one, 0, 0) for jl in range(4)]
            for quad in range(4):
                down[2 * cx + i, quad] += jnp.concatenate(
                    [p[:, 32 * quad : 32 * quad + 32] for p in pieces], axis=1
                )

    def far_x(x, carry):
        for yp in range(2):
            for zp in range(2):
                far = dot(down[x, 2 * yp + zp].astype(BF), basis[...], 0, 0)
                for y2 in range(2):
                    for z2 in range(2):
                        row = 64 * y2 + 32 * z2
                        near[
                            x, 2 * yp + y2, 32 * zp : 32 * zp + 32, 128 * z2 : 128 * z2 + 128
                        ] += far[row : row + 32]
        return carry

    lax.fori_loop(0, 4, far_x, 0, unroll=4)

    middle(0)
    for dy, (yo, count_y, yi) in INNER.items():
        ys, rows_y = pl.ds(yi, count_y), pl.ds(yo, count_y)
        for zp, z, column in ((0, 0, 0), (1, 5, 128)):
            source_z = jnp.concatenate(
                [boxes(pl.ds(dx, 4), ys, (z,)) for dx in range(3)], axis=1
            )
            taps = jnp.concatenate(
                [toep[3 * dx + dy, 384 * zp : 384 * zp + 128, column : column + 128] for dx in range(3)],
                axis=0,
            )
            value = dot(source_z, taps).reshape(4, count_y, 32, 128)
            near[:, rows_y, pl.ds(32 * zp, 32), pl.ds(column, 128)] += value
        for dx, xe, xo in ((0, 0, 0), (2, 5, 3)):
            for zp, zs, rows in ((0, (1, 2, 3), pl.ds(128, 384)), (1, (2, 3, 4), pl.ds(0, 384))):
                value = dot(boxes(pl.ds(xe, 1), ys, zs), toep[3 * dx + dy, rows])
                near[xo, rows_y, pl.ds(32 * zp, 32)] += value.reshape(count_y, 32, 256)

    def write(y):
        for x in range(4):
            for z in range(4):
                zp, z2 = z // 2, z % 2
                value = near[x, y, 32 * zp : 32 * zp + 32, 128 * z2 : 128 * z2 + 128]
                result[x, y, z] = jnp.where(lane < counts[x, y, z], value, 0.0)
        copy = pltpu.make_async_copy(result.at[:, y], out.at[:, y], out_sem.at[y])
        copy.start()
        return copy

    stores = [write(1), write(2)]

    finish(0)
    for dy, ext_y, y in ((0, 0, 0), (2, 5, 3)):
        acc = jnp.zeros((256, 256), F32)
        for step in range(3):
            rows = [
                jnp.concatenate([ext[pl.ds(step, 4), ext_y, 2 * zp + j] for j in range(4)], axis=2)
                for zp in range(2)
            ]
            acc = acc + dot(jnp.stack(rows, axis=1).reshape(256, 512), toep[3 * step + dy])
        near[:, y] += acc.reshape(4, 64, 256)
        stores.append(write(y))
    for copy in stores:
        copy.wait()

    for f in range(3):
        for group in (planes[f], slabs[f], sides[f]):
            for copy in group.values():
                copy.wait_send()

    def sent_line(d, carry):
        gather_copy(d).wait_send()
        return carry

    lax.fori_loop(1, nx, sent_line, 0)

    def sent_plane(d, carry):
        part_copy(d).wait_send()
        return carry

    lax.fori_loop(1, ny * nz, sent_plane, 0)


def body(
    sizes,
    charges,
    counts,
    near_offsets,
    near_blocks,
    leaf_basis,
    transfer,
    far_offsets,
    coupling,
    coarse_coupling,
):
    smem = pl.BlockSpec(memory_space=pltpu.SMEM)
    hbm = pl.BlockSpec(memory_space=pl.ANY)
    dma = pltpu.SemaphoreType.DMA
    nx, ny, nz = sizes
    return pl.pallas_call(
        functools.partial(kernel, sizes),
        out_shape=jax.ShapeDtypeStruct((4, 4, 4, 32, 128), F32),
        in_specs=[smem] * 3 + [hbm] * 6,
        out_specs=hbm,
        scratch_shapes=[
            pltpu.VMEM((6, 6, 6, 32, 128), BF),
            pltpu.VMEM((4, 8, 4, 4, 48, 128), BF),
            pltpu.VMEM((4, 6, 3, 3, 48, 128), BF),
            pltpu.VMEM((4, 4, 4, 32, 128), BF),
            pltpu.VMEM((27, 128, 128), BF),
            pltpu.VMEM((48, 128), BF),
            pltpu.VMEM((8, 48, 48), BF),
            pltpu.VMEM((2, 32, 48, 48), BF),
            pltpu.VMEM((16, 4, 4, 48, 48), BF),
            pltpu.VMEM((9, 512, 256), BF),
            pltpu.VMEM((2, 48, 1536), BF),
            pltpu.VMEM((4, 4, 64, 256), F32),
            pltpu.VMEM((4, 4, 4, 32, 128), F32),
            pltpu.VMEM((nx, 16, 128), BF),
            pltpu.VMEM((ny * nz, 16, 128), F32),
            pltpu.VMEM((ny * nz, 16, 128), F32),
            pltpu.VMEM((4, 4, 48, 128), F32),
            pltpu.SMEM((64,), jnp.int32),
            pltpu.SMEM((64,), jnp.int32),
            dma((6,)),
            dma((4,)),
            dma((3 * SEMS,)),
            dma((3 * SEMS,)),
            dma((nx,)),
            dma((nx,)),
            dma((ny * nz,)),
            dma((ny * nz,)),
        ],
        compiler_params=pltpu.CompilerParams(
            collective_id=0, has_side_effects=True, vmem_limit_bytes=60 * 1024 * 1024
        ),
    )(
        counts,
        near_offsets.T,
        far_offsets.transpose(2, 0, 1),
        charges,
        near_blocks,
        leaf_basis,
        transfer,
        coupling,
        coarse_coupling,
    )


def solution(mesh):
    sizes = (mesh.shape["gx"], mesh.shape["gy"], mesh.shape["gz"])
    spread = P("gx", "gy", "gz", None, None)
    in_specs = (spread, P("gx", "gy", "gz"), P(), P(), P(), P(), P(), P(), P())
    return jax.shard_map(
        functools.partial(body, sizes),
        mesh=mesh,
        in_specs=in_specs,
        out_specs=spread,
        check_vma=False,
    )
```

```python
import functools

import jax
import jax.numpy as jnp
from jax import lax
from jax.experimental import pallas as pl
from jax.experimental.pallas import tpu as pltpu
from jax.sharding import PartitionSpec as P

MESH = pl.DeviceIdType.MESH
BF = jnp.bfloat16
F32 = jnp.float32

FIELDS = (
    ((1, 5, 1), (1, 5, 1), (1, 5, 1)),
    ((2, 6, 2), (1, 3, 1), (1, 3, 1)),
    ((2, 4, 2), (1, 2, 1), (1, 2, 1)),
)
SEMS = 18


def own(axis):
    return pl.ds(axis[0], axis[1] - axis[0])


def source(axis, step):
    low, high, width = axis
    return pl.ds(high - width, width) if step > 0 else pl.ds(low, width)


def target(axis, step):
    low, high, width = axis
    return pl.ds(low - width, width) if step > 0 else pl.ds(high, width)


def dot(a, b, contract_a=1, contract_b=0):
    return lax.dot_general(
        a, b, (((contract_a,), (contract_b,)), ((), ())), preferred_element_type=F32
    )


def pack(value):
    zero = jnp.zeros((16, 32), value.dtype)
    return jnp.concatenate([value[0:16], value[16:32], value[32:48], zero], axis=1)


def unpack(value):
    return jnp.concatenate([value[:, 0:32], value[:, 32:64], value[:, 64:96]], axis=0)


def kernel(
    sizes,
    counts,
    near_off,
    far_off,
    charges,
    near_blocks,
    basis_hbm,
    transfer_hbm,
    coupling_hbm,
    coarse_hbm,
    out,
    ext,
    mom,
    one,
    raw,
    blocks,
    basis,
    transfer,
    coupling,
    coarse,
    toep,
    packed,
    near,
    result,
    gathered,
    part_out,
    part_in,
    down,
    inverse,
    base,
    in_sem,
    out_sem,
    send_sem,
    recv_sem,
    g_send,
    g_recv,
    p_send,
    p_recv,
):
    nx, ny, nz = sizes
    mx, my, mz = lax.axis_index("gx"), lax.axis_index("gy"), lax.axis_index("gz")

    odd = lax.rem(mz, 2)
    flip = 2 * odd - 1

    def device(dx, dy, dz):
        return {
            "gx": lax.rem(mx + (dx + nx), nx),
            "gy": lax.rem(my + (dy + ny), ny),
            "gz": lax.rem(mz + (dz + nz), nz),
        }

    loads = [
        pltpu.make_async_copy(src, dst, in_sem.at[i])
        for i, (src, dst) in enumerate(
            (
                (charges, raw),
                (basis_hbm, basis),
                (transfer_hbm, transfer),
                (near_blocks, blocks),
                (coarse_hbm, coarse),
                (coupling_hbm, coupling),
            )
        )
    ]
    for copy in loads:
        copy.start()

    barrier = pltpu.get_barrier_semaphore()
    for dx in (-1, 1):
        pl.semaphore_signal(barrier, inc=1, device_id=device(dx, 0, flip), device_id_type=MESH)

    def greet_line(d, carry):
        pl.semaphore_signal(barrier, inc=1, device_id=device(d, 0, 0), device_id_type=MESH)
        return carry

    lax.fori_loop(1, nx, greet_line, 0)

    def greet_plane(d, carry):
        pl.semaphore_signal(
            barrier, inc=1, device_id=device(0, d // nz, d % nz), device_id_type=MESH
        )
        return carry

    lax.fori_loop(1, ny * nz, greet_plane, 0)

    bufs = (ext, mom.at[0], one.at[0])

    def remote(f, sem, to, src, dst):
        return pltpu.make_async_remote_copy(
            src_ref=bufs[f].at[src],
            dst_ref=bufs[f].at[dst],
            send_sem=send_sem.at[SEMS * f + sem],
            recv_sem=recv_sem.at[SEMS * f + sem],
            device_id=to,
            device_id_type=MESH,
        )

    def copies(f):
        ax, ay, az = FIELDS[f]
        low, high, width = az
        span = high - low
        wide = span + width
        outer_src = pl.ds(low + odd * (span - width), width)
        inner_src = pl.ds(high - width - odd * (span - width), width)
        outer_dst = pl.ds(low - width + odd * wide, width)
        inner_dst = pl.ds(high - odd * wide, width)
        own_outer = pl.ds(low - width + odd * width, wide)
        plane = {}
        for dx in (-1, 0, 1):
            rx = (source(ax, dx), target(ax, dx)) if dx else (own(ax), own(ax))
            if dx:
                plane[dx, 0] = remote(
                    f, (dx + 1) // 2, device(dx, 0, 0),
                    (rx[0], own(ay), own(az)), (rx[1], own(ay), own(az)),
                )
            plane[dx, 1] = remote(
                f, 3 + dx, device(dx, 0, flip),
                (rx[0], own(ay), outer_src), (rx[1], own(ay), inner_dst),
            )
        slab = {}
        regions = {
            "own": (own(ax), own(az)),
            "low": (target(ax, 1), own_outer),
            "high": (target(ax, -1), own_outer),
            "outer": (own(ax), outer_dst),
        }
        for j, dy in enumerate((-1, 1)):
            for i, (name, (rx, rz)) in enumerate(regions.items()):
                slab[dy, name] = remote(
                    f, 5 + 4 * j + i, device(0, dy, 0),
                    (rx, source(ay, dy), rz), (rx, target(ay, dy), rz),
                )
        side = {}
        full = pl.ds(0, ax[1] + ax[2])
        regions = {
            "own": (own(ax), own(ay)),
            "low": (target(ax, 1), own(ay)),
            "high": (target(ax, -1), own(ay)),
            1: (full, target(ay, 1)),
            -1: (full, target(ay, -1)),
        }
        for i, (name, (rx, ry)) in enumerate(regions.items()):
            side[name] = remote(
                f, 13 + i, device(0, 0, -flip), (rx, ry, inner_src), (rx, ry, outer_dst)
            )
        return plane, slab, side

    planes, slabs, sides = zip(*[copies(f) for f in range(3)])

    def start_slab(f):
        for dy in (-1, 1):
            slabs[f][dy, "own"].start()

    def start_plane(f):
        sides[f]["own"].start()
        for step in ((-1, 0), (1, 0), (-1, 1), (1, 1), (0, 1)):
            planes[f][step].start()

    def forward(f):
        for name, dx in (("low", 1), ("high", -1)):
            planes[f][dx, 0].wait_recv()
            sides[f][name].start()
            planes[f][dx, 1].wait_recv()
            for dy in (-1, 1):
                slabs[f][dy, name].start()

    def forward_outer(f):
        planes[f][0, 1].wait_recv()
        for dy in (-1, 1):
            slabs[f][dy, "outer"].start()

    def middle(f):
        for name in ("own", "low", "high"):
            sides[f][name].wait_recv()

    def hand_over(f):
        for dy in (-1, 1):
            for name in ("own", "low", "high"):
                slabs[f][dy, name].wait_recv()
            sides[f][dy].start()

    def finish(f):
        for dy in (-1, 1):
            slabs[f][dy, "outer"].wait_recv()
            sides[f][dy].wait_recv()

    loads[0].wait()
    lane = lax.broadcasted_iota(jnp.int32, (32, 128), 1)

    def mask_x(x, carry):
        for y in range(4):
            for z in range(4):
                live = (lane < counts[x, y, z]).astype(F32).astype(BF)
                ext[x + 1, y + 1, z + 1] = raw[x, y, z] * live
        return carry

    lax.fori_loop(0, 4, mask_x, 0)

    loads[1].wait()
    loads[2].wait()

    def leaf_x(x, carry):
        for yp in range(2):
            for zp in range(2):
                box = ext[x + 1, pl.ds(2 * yp + 1, 2), pl.ds(2 * zp + 1, 2)]
                value = dot(basis[...], box.reshape(128, 128), 1, 1)
                mom[0, x + 2, yp + 1, zp + 1] = value.astype(BF)
        return carry

    lax.fori_loop(0, 4, leaf_x, 0)

    for cx in range(2):
        acc = jnp.zeros((48, 128), F32)
        for i in range(2):
            quads = [mom[0, 2 * cx + i + 2, cy + 1, cz + 1] for cy in range(2) for cz in range(2)]
            for jl in range(4):
                kids = jnp.concatenate([q[:, 32 * jl : 32 * jl + 32] for q in quads], axis=1)
                acc = acc + dot(transfer[4 * i + jl], kids)
        one[0, cx + 2, 1, 1] = acc.astype(BF)

    acc = jnp.zeros((48, 32), F32)
    for i in range(2):
        box = one[0, i + 2, 1, 1]
        for jl in range(4):
            acc = acc + dot(transfer[4 * i + jl], box[:, 32 * jl : 32 * jl + 32])
    gathered[0] = pack(acc).astype(BF)

    def gather_copy(d):
        return pltpu.make_async_remote_copy(
            src_ref=gathered.at[0],
            dst_ref=gathered.at[d],
            send_sem=g_send.at[d],
            recv_sem=g_recv.at[d],
            device_id=device(d, 0, 0),
            device_id_type=MESH,
        )

    def gather_start(d, carry):
        gather_copy(d).start()
        return carry

    pl.semaphore_wait(barrier, (nx - 1) + (ny * nz - 1) + 2)
    lax.fori_loop(1, nx, gather_start, 0)
    start_plane(1)
    start_slab(1)
    start_plane(2)
    start_slab(2)
    start_slab(0)

    codes = [9 * near_off[0, s] + 3 * near_off[1, s] + near_off[2, s] + 13 for s in range(27)]
    for s in range(27):
        inverse[27 + s] = codes[s]

    def invert(c, carry):
        found = jnp.int32(0)
        for s in range(27):
            found = jnp.where(inverse[27 + s] == c, jnp.int32(s), found)
        inverse[c] = found
        return carry

    lax.fori_loop(0, 27, invert, 0)
    for level in range(2):
        for e in range(32):
            ox = far_off[0, level, e] + 2
            ay = far_off[1, level, e] + 2
            az = far_off[2, level, e] + 2
            half_y, half_z = lax.shift_right_logical(ay, 1), lax.shift_right_logical(az, 1)
            kind = 2 * (ay - 2 * half_y) + (az - 2 * half_z)
            if level == 0:
                base[e] = ((kind * 8 + ox) * 4 + half_y) * 4 + half_z
            else:
                base[32 + e] = ((kind * 6 + ox) * 3 + half_y) * 3 + half_z

    loads[4].wait()

    def gather_wait(d, carry):
        gather_copy(d).wait_recv()
        return carry

    lax.fori_loop(1, nx, gather_wait, 0)

    def partial(dy, carry):
        acc = jnp.zeros((192, 32), F32)
        for d in range(nx):
            mats = coarse[(nx - d) % nx, dy].reshape(192, 48)
            acc = acc + dot(mats, unpack(gathered[d]))
        for dz in range(4):
            part_out[4 * dy + dz] = pack(acc[48 * dz : 48 * dz + 48]).astype(BF)
        return carry

    lax.fori_loop(0, 4, partial, 0)

    def part_copy(d):
        return pltpu.make_async_remote_copy(
            src_ref=part_out.at[d],
            dst_ref=part_in.at[d],
            send_sem=p_send.at[d],
            recv_sem=p_recv.at[d],
            device_id=device(0, -(d // nz), -(d % nz)),
            device_id_type=MESH,
        )

    def part_start(d, carry):
        part_copy(d).start()
        return carry

    lax.fori_loop(1, ny * nz, part_start, 0)
    start_plane(0)

    loads[3].wait()

    def build(c, carry):
        taps = [blocks[inverse[3 * c + t]].T for t in range(3)]
        zero = jnp.zeros((128, 128), BF)
        toep[c, 0:128, 0:128] = taps[0]
        toep[c, 0:128, 128:256] = zero
        toep[c, 128:256, 0:128] = taps[1]
        toep[c, 128:256, 128:256] = taps[0]
        toep[c, 256:384, 0:128] = taps[2]
        toep[c, 256:384, 128:256] = taps[1]
        toep[c, 384:512, 0:128] = zero
        toep[c, 384:512, 128:256] = taps[2]
        return carry

    lax.fori_loop(0, 9, build, 0)

    loads[5].wait()
    for level in range(2):
        for e in range(32):
            packed[level, :, 48 * e : 48 * e + 48] = coupling[level, e]

    def boxes(xs, ys, zs):
        parts = [ext[xs, ys, z] for z in zs]
        rows = parts[0].shape[0] * parts[0].shape[1] * 32
        return jnp.concatenate(parts, axis=3).reshape(rows, 128 * len(zs))

    INNER = {1: (0, 4, 1), 0: (1, 3, 1), 2: (0, 3, 2)}
    for dx, (xo, count_x, xi) in INNER.items():
        for dy, (yo, count_y, yi) in INNER.items():
            for zp, zs, rows in ((0, (1, 2, 3), pl.ds(128, 384)), (1, (2, 3, 4), pl.ds(0, 384))):
                value = dot(
                    boxes(pl.ds(xi, count_x), pl.ds(yi, count_y), zs), toep[3 * dx + dy, rows]
                ).reshape(count_x, count_y, 32, 256)
                at = (pl.ds(xo, count_x), pl.ds(yo, count_y), pl.ds(32 * zp, 32))
                if (dx, dy) == (1, 1):
                    near[at] = value
                else:
                    near[at] += value


    group = lax.broadcasted_iota(jnp.int32, (48, 128), 1)
    even_z = (group % 64) < 32
    first_y = group < 64

    def ahead_y(a, b):
        return jnp.where(first_y, pltpu.roll(a, 64, 1), pltpu.roll(b, 64, 1))

    def shifts(buf, side, x, inner):
        middle_rows = range(1, side - 1)
        for yp in range(side):
            if (yp in middle_rows) == inner:
                line = [buf[0, x, yp, zp] for zp in range(side)]
                down_z = [pltpu.roll(v, 96, 1) for v in line[:-1]]
                up_z = [pltpu.roll(v, 32, 1) for v in line[1:]]
                for zp in range(side - 1):
                    buf[1, x, yp, zp] = jnp.where(even_z, down_z[zp], up_z[zp])
        for yp in range(side - 1):
            if (yp in middle_rows and yp + 1 in middle_rows) == inner:
                for zp in range(side):
                    buf[2, x, yp, zp] = ahead_y(buf[0, x, yp, zp], buf[0, x, yp + 1, zp])
                for zp in range(side - 1):
                    buf[3, x, yp, zp] = ahead_y(buf[1, x, yp, zp], buf[1, x, yp + 1, zp])

    def shift_all(buf, planes_x, side, inner):
        def step(x, carry):
            shifts(buf, side, x, inner)
            return carry

        lax.fori_loop(0, planes_x, step, 0, unroll=planes_x // 2)

    forward(1)
    forward_outer(1)
    forward(2)
    forward_outer(2)
    middle(1)
    shift_all(mom, 8, 4, True)
    middle(2)
    shift_all(one, 6, 3, True)
    hand_over(1)
    forward(0)

    for dy, (yo, count_y, yi) in INNER.items():
        ys, rows_y = pl.ds(yi, count_y), pl.ds(yo, count_y)
        for dx, xe, xo in ((0, 0, 0), (2, 5, 3)):
            for zp, zs, rows in ((0, (1, 2, 3), pl.ds(128, 384)), (1, (2, 3, 4), pl.ds(0, 384))):
                value = dot(boxes(pl.ds(xe, 1), ys, zs), toep[3 * dx + dy, rows])
                near[xo, rows_y, pl.ds(32 * zp, 32)] += value.reshape(count_y, 32, 256)

    finish(1)
    shift_all(mom, 8, 4, False)
    forward_outer(0)
    hand_over(2)
    flat_mom = mom.reshape(4 * 8 * 4 * 4, 48, 128)

    def leaf_list(t, carry):
        x, yp = t // 2, t % 2
        offset = x * 16 + yp * 4
        windows = [
            jnp.concatenate([flat_mom[base[e] + (offset + zp)] for e in range(32)], axis=0)
            for zp in range(2)
        ]
        local = dot(packed[0], jnp.concatenate(windows, axis=1))
        for zp in range(2):
            down[x, 2 * yp + zp] = local[:, 128 * zp : 128 * zp + 128]
        return carry

    lax.fori_loop(0, 4, leaf_list, 0, unroll=4)
    hand_over(0)
    lax.fori_loop(4, 8, leaf_list, 0, unroll=4)

    finish(2)

    shift_all(one, 6, 3, False)
    flat_one = one.reshape(4 * 6 * 3 * 3, 48, 128)
    windows = [
        jnp.concatenate([flat_one[base[32 + e] + cx * 9] for e in range(32)], axis=0)
        for cx in range(2)
    ]
    local_one = dot(packed[1], jnp.concatenate(windows, axis=1))

    def part_wait(d, carry):
        part_copy(d).wait_recv()
        return carry

    lax.fori_loop(1, ny * nz, part_wait, 0)
    total = part_out[0].astype(F32)
    for d in range(1, ny * nz):
        total = total + part_in[d].astype(F32)
    local_two = unpack(total).astype(BF)
    for cx in range(2):
        spread = jnp.concatenate(
            [dot(transfer[4 * cx + jl], local_two, 0, 0) for jl in range(4)], axis=1
        )
        total_one = (local_one[:, 128 * cx : 128 * cx + 128] + spread).astype(BF)
        for i in range(2):
            pieces = [dot(transfer[4 * i + jl], total_one, 0, 0) for jl in range(4)]
            for quad in range(4):
                down[2 * cx + i, quad] += jnp.concatenate(
                    [p[:, 32 * quad : 32 * quad + 32] for p in pieces], axis=1
                )

    def far_x(x, carry):
        for yp in range(2):
            for zp in range(2):
                far = dot(down[x, 2 * yp + zp].astype(BF), basis[...], 0, 0)
                for y2 in range(2):
                    for z2 in range(2):
                        row = 64 * y2 + 32 * z2
                        near[
                            x, 2 * yp + y2, 32 * zp : 32 * zp + 32, 128 * z2 : 128 * z2 + 128
                        ] += far[row : row + 32]
        return carry

    lax.fori_loop(0, 4, far_x, 0, unroll=4)

    middle(0)
    for dy, (yo, count_y, yi) in INNER.items():
        ys, rows_y = pl.ds(yi, count_y), pl.ds(yo, count_y)
        for zp, z, column in ((0, 0, 0), (1, 5, 128)):
            source_z = jnp.concatenate(
                [boxes(pl.ds(dx, 4), ys, (z,)) for dx in range(3)], axis=1
            )
            taps = jnp.concatenate(
                [toep[3 * dx + dy, 384 * zp : 384 * zp + 128, column : column + 128] for dx in range(3)],
                axis=0,
            )
            value = dot(source_z, taps).reshape(4, count_y, 32, 128)
            near[:, rows_y, pl.ds(32 * zp, 32), pl.ds(column, 128)] += value

    def write(y):
        for x in range(4):
            for z in range(4):
                zp, z2 = z // 2, z % 2
                value = near[x, y, 32 * zp : 32 * zp + 32, 128 * z2 : 128 * z2 + 128]
                result[x, y, z] = jnp.where(lane < counts[x, y, z], value, 0.0)
        copy = pltpu.make_async_copy(result.at[:, y], out.at[:, y], out_sem.at[y])
        copy.start()
        return copy

    stores = [write(1), write(2)]

    finish(0)
    for dy, ext_y, y in ((0, 0, 0), (2, 5, 3)):
        acc = jnp.zeros((256, 256), F32)
        for step in range(3):
            rows = [
                jnp.concatenate([ext[pl.ds(step, 4), ext_y, 2 * zp + j] for j in range(4)], axis=2)
                for zp in range(2)
            ]
            acc = acc + dot(jnp.stack(rows, axis=1).reshape(256, 512), toep[3 * step + dy])
        near[:, y] += acc.reshape(4, 64, 256)
        stores.append(write(y))
    for copy in stores:
        copy.wait()

    for f in range(3):
        for group in (planes[f], slabs[f], sides[f]):
            for copy in group.values():
                copy.wait_send()

    def sent_line(d, carry):
        gather_copy(d).wait_send()
        return carry

    lax.fori_loop(1, nx, sent_line, 0)

    def sent_plane(d, carry):
        part_copy(d).wait_send()
        return carry

    lax.fori_loop(1, ny * nz, sent_plane, 0)


def body(
    sizes,
    charges,
    counts,
    near_offsets,
    near_blocks,
    leaf_basis,
    transfer,
    far_offsets,
    coupling,
    coarse_coupling,
):
    smem = pl.BlockSpec(memory_space=pltpu.SMEM)
    hbm = pl.BlockSpec(memory_space=pl.ANY)
    dma = pltpu.SemaphoreType.DMA
    nx, ny, nz = sizes
    return pl.pallas_call(
        functools.partial(kernel, sizes),
        out_shape=jax.ShapeDtypeStruct((4, 4, 4, 32, 128), F32),
        in_specs=[smem] * 3 + [hbm] * 6,
        out_specs=hbm,
        scratch_shapes=[
            pltpu.VMEM((6, 6, 6, 32, 128), BF),
            pltpu.VMEM((4, 8, 4, 4, 48, 128), BF),
            pltpu.VMEM((4, 6, 3, 3, 48, 128), BF),
            pltpu.VMEM((4, 4, 4, 32, 128), BF),
            pltpu.VMEM((27, 128, 128), BF),
            pltpu.VMEM((48, 128), BF),
            pltpu.VMEM((8, 48, 48), BF),
            pltpu.VMEM((2, 32, 48, 48), BF),
            pltpu.VMEM((16, 4, 4, 48, 48), BF),
            pltpu.VMEM((9, 512, 256), BF),
            pltpu.VMEM((2, 48, 1536), BF),
            pltpu.VMEM((4, 4, 64, 256), F32),
            pltpu.VMEM((4, 4, 4, 32, 128), F32),
            pltpu.VMEM((nx, 16, 128), BF),
            pltpu.VMEM((ny * nz, 16, 128), BF),
            pltpu.VMEM((ny * nz, 16, 128), BF),
            pltpu.VMEM((4, 4, 48, 128), F32),
            pltpu.SMEM((64,), jnp.int32),
            pltpu.SMEM((64,), jnp.int32),
            dma((6,)),
            dma((4,)),
            dma((3 * SEMS,)),
            dma((3 * SEMS,)),
            dma((nx,)),
            dma((nx,)),
            dma((ny * nz,)),
            dma((ny * nz,)),
        ],
        compiler_params=pltpu.CompilerParams(
            collective_id=0, has_side_effects=True, vmem_limit_bytes=60 * 1024 * 1024
        ),
    )(
        counts,
        near_offsets.T,
        far_offsets.transpose(2, 0, 1),
        charges,
        near_blocks,
        leaf_basis,
        transfer,
        coupling,
        coarse_coupling,
    )


def solution(mesh):
    sizes = (mesh.shape["gx"], mesh.shape["gy"], mesh.shape["gz"])
    spread = P("gx", "gy", "gz", None, None)
    in_specs = (spread, P("gx", "gy", "gz"), P(), P(), P(), P(), P(), P(), P())
    return jax.shard_map(
        functools.partial(body, sizes),
        mesh=mesh,
        in_specs=in_specs,
        out_specs=spread,
        check_vma=False,
    )
```

```python
import functools

import jax
import jax.numpy as jnp
from jax import lax
from jax.experimental import pallas as pl
from jax.experimental.pallas import tpu as pltpu
from jax.sharding import PartitionSpec as P

MESH = pl.DeviceIdType.MESH
BF = jnp.bfloat16
F32 = jnp.float32

FIELDS = (
    ((1, 5, 1), (1, 5, 1), (1, 5, 1)),
    ((2, 6, 2), (1, 3, 1), (1, 3, 1)),
    ((2, 4, 2), (1, 2, 1), (1, 2, 1)),
)
SEMS = 18


def own(axis):
    return pl.ds(axis[0], axis[1] - axis[0])


def source(axis, step):
    low, high, width = axis
    return pl.ds(high - width, width) if step > 0 else pl.ds(low, width)


def target(axis, step):
    low, high, width = axis
    return pl.ds(low - width, width) if step > 0 else pl.ds(high, width)


def dot(a, b, contract_a=1, contract_b=0):
    return lax.dot_general(
        a, b, (((contract_a,), (contract_b,)), ((), ())), preferred_element_type=F32
    )


def pack(value):
    zero = jnp.zeros((16, 32), value.dtype)
    return jnp.concatenate([value[0:16], value[16:32], value[32:48], zero], axis=1)


def unpack(value):
    return jnp.concatenate([value[:, 0:32], value[:, 32:64], value[:, 64:96]], axis=0)


def kernel(
    sizes,
    counts,
    near_off,
    far_off,
    charges,
    near_blocks,
    basis_hbm,
    transfer_hbm,
    coupling_hbm,
    coarse_hbm,
    out,
    ext,
    mom,
    one,
    raw,
    blocks,
    basis,
    transfer,
    coupling,
    coarse,
    toep,
    packed,
    near,
    result,
    gathered,
    part_out,
    part_in,
    down,
    inverse,
    base,
    in_sem,
    out_sem,
    send_sem,
    recv_sem,
    g_send,
    g_recv,
    p_send,
    p_recv,
):
    nx, ny, nz = sizes
    mx, my, mz = lax.axis_index("gx"), lax.axis_index("gy"), lax.axis_index("gz")

    odd = lax.rem(mz, 2)
    flip = 2 * odd - 1

    def device(dx, dy, dz):
        return {
            "gx": lax.rem(mx + (dx + nx), nx),
            "gy": lax.rem(my + (dy + ny), ny),
            "gz": lax.rem(mz + (dz + nz), nz),
        }

    loads = [
        pltpu.make_async_copy(src, dst, in_sem.at[i])
        for i, (src, dst) in enumerate(
            (
                (charges, raw),
                (basis_hbm, basis),
                (transfer_hbm, transfer),
                (near_blocks, blocks),
                (coarse_hbm, coarse),
                (coupling_hbm, coupling),
            )
        )
    ]
    for copy in loads[:3]:
        copy.start()

    barrier = pltpu.get_barrier_semaphore()
    for dx in (-1, 1):
        pl.semaphore_signal(barrier, inc=1, device_id=device(dx, 0, flip), device_id_type=MESH)

    def greet_line(d, carry):
        pl.semaphore_signal(barrier, inc=1, device_id=device(d, 0, 0), device_id_type=MESH)
        return carry

    lax.fori_loop(1, nx, greet_line, 0)

    def greet_plane(d, carry):
        pl.semaphore_signal(
            barrier, inc=1, device_id=device(0, d // nz, d % nz), device_id_type=MESH
        )
        return carry

    lax.fori_loop(1, ny * nz, greet_plane, 0)

    bufs = (ext, mom.at[0], one.at[0])

    def remote(f, sem, to, src, dst):
        return pltpu.make_async_remote_copy(
            src_ref=bufs[f].at[src],
            dst_ref=bufs[f].at[dst],
            send_sem=send_sem.at[SEMS * f + sem],
            recv_sem=recv_sem.at[SEMS * f + sem],
            device_id=to,
            device_id_type=MESH,
        )

    def copies(f):
        ax, ay, az = FIELDS[f]
        low, high, width = az
        span = high - low
        wide = span + width
        outer_src = pl.ds(low + odd * (span - width), width)
        inner_src = pl.ds(high - width - odd * (span - width), width)
        outer_dst = pl.ds(low - width + odd * wide, width)
        inner_dst = pl.ds(high - odd * wide, width)
        own_outer = pl.ds(low - width + odd * width, wide)
        plane = {}
        for dx in (-1, 0, 1):
            rx = (source(ax, dx), target(ax, dx)) if dx else (own(ax), own(ax))
            far = rx
            if f == 2 and dx:
                far = (pl.ds(2, 1), pl.ds(0, 1)) if dx > 0 else (pl.ds(3, 1), pl.ds(5, 1))
            if dx:
                plane[dx, 0] = remote(
                    f, (dx + 1) // 2, device(dx, 0, 0),
                    (far[0], own(ay), own(az)), (far[1], own(ay), own(az)),
                )
            plane[dx, 1] = remote(
                f, 3 + dx, device(dx, 0, flip),
                (rx[0], own(ay), outer_src), (rx[1], own(ay), inner_dst),
            )
        slab = {}
        regions = {
            "own": (own(ax), own(az)),
            "low": (target(ax, 1), own_outer),
            "high": (target(ax, -1), own_outer),
            "outer": (own(ax), outer_dst),
        }
        for j, dy in enumerate((-1, 1)):
            for i, (name, (rx, rz)) in enumerate(regions.items()):
                slab[dy, name] = remote(
                    f, 5 + 4 * j + i, device(0, dy, 0),
                    (rx, source(ay, dy), rz), (rx, target(ay, dy), rz),
                )
        side = {}
        full = pl.ds(0, ax[1] + ax[2])
        regions = {
            "own": (own(ax), own(ay)),
            "low": (target(ax, 1), own(ay)),
            "high": (target(ax, -1), own(ay)),
            1: (full, target(ay, 1)),
            -1: (full, target(ay, -1)),
        }
        for i, (name, (rx, ry)) in enumerate(regions.items()):
            side[name] = remote(
                f, 13 + i, device(0, 0, -flip), (rx, ry, inner_src), (rx, ry, outer_dst)
            )
        return plane, slab, side

    planes, slabs, sides = zip(*[copies(f) for f in range(3)])

    def start_slab(f):
        for dy in (-1, 1):
            slabs[f][dy, "own"].start()

    def start_plane(f):
        sides[f]["own"].start()
        for step in ((-1, 0), (1, 0), (-1, 1), (1, 1), (0, 1)):
            planes[f][step].start()

    def forward(f):
        for name, dx in (("low", 1), ("high", -1)):
            planes[f][dx, 0].wait_recv()
            sides[f][name].start()
            planes[f][dx, 1].wait_recv()
            for dy in (-1, 1):
                slabs[f][dy, name].start()

    def forward_outer(f):
        planes[f][0, 1].wait_recv()
        for dy in (-1, 1):
            slabs[f][dy, "outer"].start()

    def middle(f):
        for name in ("own", "low", "high"):
            sides[f][name].wait_recv()

    def hand_over(f):
        for dy in (-1, 1):
            for name in ("own", "low", "high"):
                slabs[f][dy, name].wait_recv()
            sides[f][dy].start()

    def finish(f):
        for dy in (-1, 1):
            slabs[f][dy, "outer"].wait_recv()
            sides[f][dy].wait_recv()

    loads[0].wait()
    for copy in loads[3:]:
        copy.start()
    lane = lax.broadcasted_iota(jnp.int32, (32, 128), 1)

    def mask_x(x, carry):
        for y in range(4):
            for z in range(4):
                live = (lane < counts[x, y, z]).astype(F32).astype(BF)
                ext[x + 1, y + 1, z + 1] = raw[x, y, z] * live
        return carry

    lax.fori_loop(0, 4, mask_x, 0)

    loads[1].wait()
    loads[2].wait()

    def leaf_x(x, carry):
        for yp in range(2):
            for zp in range(2):
                box = ext[x + 1, pl.ds(2 * yp + 1, 2), pl.ds(2 * zp + 1, 2)]
                value = dot(basis[...], box.reshape(128, 128), 1, 1)
                mom[0, x + 2, yp + 1, zp + 1] = value.astype(BF)
        return carry

    lax.fori_loop(0, 4, leaf_x, 0)

    def merge(x):
        acc = jnp.zeros((48, 128), F32)
        for i in range(2):
            quads = [mom[0, 2 * x - 2 + i, cy + 1, cz + 1] for cy in range(2) for cz in range(2)]
            for jl in range(4):
                kids = jnp.concatenate([q[:, 32 * jl : 32 * jl + 32] for q in quads], axis=1)
                acc = acc + dot(transfer[4 * i + jl], kids)
        one[0, x, 1, 1] = acc.astype(BF)

    for x in (2, 3):
        merge(x)

    acc = jnp.zeros((48, 32), F32)
    for i in range(2):
        box = one[0, i + 2, 1, 1]
        for jl in range(4):
            acc = acc + dot(transfer[4 * i + jl], box[:, 32 * jl : 32 * jl + 32])
    gathered[0] = pack(acc).astype(BF)

    def gather_copy(d):
        return pltpu.make_async_remote_copy(
            src_ref=gathered.at[0],
            dst_ref=gathered.at[d],
            send_sem=g_send.at[d],
            recv_sem=g_recv.at[d],
            device_id=device(d, 0, 0),
            device_id_type=MESH,
        )

    def gather_start(d, carry):
        gather_copy(d).start()
        return carry

    pl.semaphore_wait(barrier, (nx - 1) + (ny * nz - 1) + 2)
    lax.fori_loop(1, nx, gather_start, 0)
    start_plane(1)
    start_slab(1)
    start_plane(2)
    start_slab(2)
    start_slab(0)

    codes = [9 * near_off[0, s] + 3 * near_off[1, s] + near_off[2, s] + 13 for s in range(27)]
    for s in range(27):
        inverse[27 + s] = codes[s]

    def invert(c, carry):
        found = jnp.int32(0)
        for s in range(27):
            found = jnp.where(inverse[27 + s] == c, jnp.int32(s), found)
        inverse[c] = found
        return carry

    lax.fori_loop(0, 27, invert, 0)
    for level in range(2):
        for e in range(32):
            ox = far_off[0, level, e] + 2
            ay = far_off[1, level, e] + 2
            az = far_off[2, level, e] + 2
            half_y, half_z = lax.shift_right_logical(ay, 1), lax.shift_right_logical(az, 1)
            kind = 2 * (ay - 2 * half_y) + (az - 2 * half_z)
            if level == 0:
                base[e] = ((kind * 8 + ox) * 4 + half_y) * 4 + half_z
            else:
                base[32 + e] = ((kind * 6 + ox) * 3 + half_y) * 3 + half_z

    loads[4].wait()

    def gather_wait(d, carry):
        gather_copy(d).wait_recv()
        return carry

    lax.fori_loop(1, nx, gather_wait, 0)

    def partial(dy, carry):
        acc = jnp.zeros((192, 32), F32)
        for d in range(nx):
            mats = coarse[(nx - d) % nx, dy].reshape(192, 48)
            acc = acc + dot(mats, unpack(gathered[d]))
        for dz in range(4):
            part_out[4 * dy + dz] = pack(acc[48 * dz : 48 * dz + 48]).astype(BF)
        return carry

    lax.fori_loop(0, 4, partial, 0)

    def part_copy(d):
        return pltpu.make_async_remote_copy(
            src_ref=part_out.at[d],
            dst_ref=part_in.at[d],
            send_sem=p_send.at[d],
            recv_sem=p_recv.at[d],
            device_id=device(0, -(d // nz), -(d % nz)),
            device_id_type=MESH,
        )

    def part_start(d, carry):
        part_copy(d).start()
        return carry

    lax.fori_loop(1, ny * nz, part_start, 0)
    start_plane(0)

    loads[3].wait()

    def build(c, carry):
        taps = [blocks[inverse[3 * c + t]].T for t in range(3)]
        zero = jnp.zeros((128, 128), BF)
        toep[c, 0:128, 0:128] = taps[0]
        toep[c, 0:128, 128:256] = zero
        toep[c, 128:256, 0:128] = taps[1]
        toep[c, 128:256, 128:256] = taps[0]
        toep[c, 256:384, 0:128] = taps[2]
        toep[c, 256:384, 128:256] = taps[1]
        toep[c, 384:512, 0:128] = zero
        toep[c, 384:512, 128:256] = taps[2]
        return carry

    lax.fori_loop(0, 9, build, 0)

    loads[5].wait()
    for level in range(2):
        for e in range(32):
            packed[level, :, 48 * e : 48 * e + 48] = coupling[level, e]

    def boxes(xs, ys, zs):
        parts = [ext[xs, ys, z] for z in zs]
        rows = parts[0].shape[0] * parts[0].shape[1] * 32
        return jnp.concatenate(parts, axis=3).reshape(rows, 128 * len(zs))

    INNER = {1: (0, 4, 1), 0: (1, 3, 1), 2: (0, 3, 2)}
    for dx, (xo, count_x, xi) in INNER.items():
        for dy, (yo, count_y, yi) in INNER.items():
            for zp, zs, rows in ((0, (1, 2, 3), pl.ds(128, 384)), (1, (2, 3, 4), pl.ds(0, 384))):
                value = dot(
                    boxes(pl.ds(xi, count_x), pl.ds(yi, count_y), zs), toep[3 * dx + dy, rows]
                ).reshape(count_x, count_y, 32, 256)
                at = (pl.ds(xo, count_x), pl.ds(yo, count_y), pl.ds(32 * zp, 32))
                if (dx, dy) == (1, 1):
                    near[at] = value
                else:
                    near[at] += value


    group = lax.broadcasted_iota(jnp.int32, (48, 128), 1)
    even_z = (group % 64) < 32
    first_y = group < 64

    def ahead_y(a, b):
        return jnp.where(first_y, pltpu.roll(a, 64, 1), pltpu.roll(b, 64, 1))

    def shifts(buf, side, x, inner):
        middle_rows = range(1, side - 1)
        for yp in range(side):
            if (yp in middle_rows) == inner:
                line = [buf[0, x, yp, zp] for zp in range(side)]
                down_z = [pltpu.roll(v, 96, 1) for v in line[:-1]]
                up_z = [pltpu.roll(v, 32, 1) for v in line[1:]]
                for zp in range(side - 1):
                    buf[1, x, yp, zp] = jnp.where(even_z, down_z[zp], up_z[zp])
        for yp in range(side - 1):
            if (yp in middle_rows and yp + 1 in middle_rows) == inner:
                for zp in range(side):
                    buf[2, x, yp, zp] = ahead_y(buf[0, x, yp, zp], buf[0, x, yp + 1, zp])
                for zp in range(side - 1):
                    buf[3, x, yp, zp] = ahead_y(buf[1, x, yp, zp], buf[1, x, yp + 1, zp])

    def shift_all(buf, planes_x, side, inner):
        def step(x, carry):
            shifts(buf, side, x, inner)
            return carry

        lax.fori_loop(0, planes_x, step, 0, unroll=planes_x // 2)

    forward(1)
    forward_outer(1)
    for x in (1, 4):
        merge(x)
    forward(2)
    forward_outer(2)
    middle(1)
    shift_all(mom, 8, 4, True)
    middle(2)
    shift_all(one, 6, 3, True)
    hand_over(1)
    forward(0)

    for dy, (yo, count_y, yi) in INNER.items():
        ys, rows_y = pl.ds(yi, count_y), pl.ds(yo, count_y)
        for dx, xe, xo in ((0, 0, 0), (2, 5, 3)):
            for zp, zs, rows in ((0, (1, 2, 3), pl.ds(128, 384)), (1, (2, 3, 4), pl.ds(0, 384))):
                value = dot(boxes(pl.ds(xe, 1), ys, zs), toep[3 * dx + dy, rows])
                near[xo, rows_y, pl.ds(32 * zp, 32)] += value.reshape(count_y, 32, 256)

    finish(1)
    shift_all(mom, 8, 4, False)
    forward_outer(0)
    hand_over(2)
    flat_mom = mom.reshape(4 * 8 * 4 * 4, 48, 128)

    def leaf_list(t, carry):
        x, yp = t // 2, t % 2
        offset = x * 16 + yp * 4
        windows = [
            jnp.concatenate([flat_mom[base[e] + (offset + zp)] for e in range(32)], axis=0)
            for zp in range(2)
        ]
        local = dot(packed[0], jnp.concatenate(windows, axis=1))
        for zp in range(2):
            down[x, 2 * yp + zp] = local[:, 128 * zp : 128 * zp + 128]
        return carry

    lax.fori_loop(0, 4, leaf_list, 0, unroll=4)
    hand_over(0)
    lax.fori_loop(4, 8, leaf_list, 0, unroll=4)

    finish(2)

    shift_all(one, 6, 3, False)
    flat_one = one.reshape(4 * 6 * 3 * 3, 48, 128)
    windows = [
        jnp.concatenate([flat_one[base[32 + e] + cx * 9] for e in range(32)], axis=0)
        for cx in range(2)
    ]
    local_one = dot(packed[1], jnp.concatenate(windows, axis=1))

    def part_wait(d, carry):
        part_copy(d).wait_recv()
        return carry

    lax.fori_loop(1, ny * nz, part_wait, 0)
    total = part_out[0].astype(F32)
    for d in range(1, ny * nz):
        total = total + part_in[d].astype(F32)
    local_two = unpack(total).astype(BF)
    for cx in range(2):
        spread = jnp.concatenate(
            [dot(transfer[4 * cx + jl], local_two, 0, 0) for jl in range(4)], axis=1
        )
        total_one = (local_one[:, 128 * cx : 128 * cx + 128] + spread).astype(BF)
        for i in range(2):
            pieces = [dot(transfer[4 * i + jl], total_one, 0, 0) for jl in range(4)]
            for quad in range(4):
                down[2 * cx + i, quad] += jnp.concatenate(
                    [p[:, 32 * quad : 32 * quad + 32] for p in pieces], axis=1
                )

    def far_x(x, carry):
        for yp in range(2):
            for zp in range(2):
                far = dot(down[x, 2 * yp + zp].astype(BF), basis[...], 0, 0)
                for y2 in range(2):
                    for z2 in range(2):
                        row = 64 * y2 + 32 * z2
                        near[
                            x, 2 * yp + y2, 32 * zp : 32 * zp + 32, 128 * z2 : 128 * z2 + 128
                        ] += far[row : row + 32]
        return carry

    lax.fori_loop(0, 4, far_x, 0, unroll=4)

    middle(0)
    for dy, (yo, count_y, yi) in INNER.items():
        ys, rows_y = pl.ds(yi, count_y), pl.ds(yo, count_y)
        for zp, z, column in ((0, 0, 0), (1, 5, 128)):
            source_z = jnp.concatenate(
                [boxes(pl.ds(dx, 4), ys, (z,)) for dx in range(3)], axis=1
            )
            taps = jnp.concatenate(
                [toep[3 * dx + dy, 384 * zp : 384 * zp + 128, column : column + 128] for dx in range(3)],
                axis=0,
            )
            value = dot(source_z, taps).reshape(4, count_y, 32, 128)
            near[:, rows_y, pl.ds(32 * zp, 32), pl.ds(column, 128)] += value

    def write(y):
        for x in range(4):
            for z in range(4):
                zp, z2 = z // 2, z % 2
                value = near[x, y, 32 * zp : 32 * zp + 32, 128 * z2 : 128 * z2 + 128]
                result[x, y, z] = jnp.where(lane < counts[x, y, z], value, 0.0)
        copy = pltpu.make_async_copy(result.at[:, y], out.at[:, y], out_sem.at[y])
        copy.start()
        return copy

    stores = [write(1), write(2)]

    finish(0)
    for dy, ext_y, y in ((0, 0, 0), (2, 5, 3)):
        acc = jnp.zeros((256, 256), F32)
        for step in range(3):
            rows = [
                jnp.concatenate([ext[pl.ds(step, 4), ext_y, 2 * zp + j] for j in range(4)], axis=2)
                for zp in range(2)
            ]
            acc = acc + dot(jnp.stack(rows, axis=1).reshape(256, 512), toep[3 * step + dy])
        near[:, y] += acc.reshape(4, 64, 256)
        stores.append(write(y))
    for copy in stores:
        copy.wait()

    for f in range(3):
        for group in (planes[f], slabs[f], sides[f]):
            for copy in group.values():
                copy.wait_send()

    def sent_line(d, carry):
        gather_copy(d).wait_send()
        return carry

    lax.fori_loop(1, nx, sent_line, 0)

    def sent_plane(d, carry):
        part_copy(d).wait_send()
        return carry

    lax.fori_loop(1, ny * nz, sent_plane, 0)


def body(
    sizes,
    charges,
    counts,
    near_offsets,
    near_blocks,
    leaf_basis,
    transfer,
    far_offsets,
    coupling,
    coarse_coupling,
):
    smem = pl.BlockSpec(memory_space=pltpu.SMEM)
    hbm = pl.BlockSpec(memory_space=pl.ANY)
    dma = pltpu.SemaphoreType.DMA
    nx, ny, nz = sizes
    return pl.pallas_call(
        functools.partial(kernel, sizes),
        out_shape=jax.ShapeDtypeStruct((4, 4, 4, 32, 128), F32),
        in_specs=[smem] * 3 + [hbm] * 6,
        out_specs=hbm,
        scratch_shapes=[
            pltpu.VMEM((6, 6, 6, 32, 128), BF),
            pltpu.VMEM((4, 8, 4, 4, 48, 128), BF),
            pltpu.VMEM((4, 6, 3, 3, 48, 128), BF),
            pltpu.VMEM((4, 4, 4, 32, 128), BF),
            pltpu.VMEM((27, 128, 128), BF),
            pltpu.VMEM((48, 128), BF),
            pltpu.VMEM((8, 48, 48), BF),
            pltpu.VMEM((2, 32, 48, 48), BF),
            pltpu.VMEM((16, 4, 4, 48, 48), BF),
            pltpu.VMEM((9, 512, 256), BF),
            pltpu.VMEM((2, 48, 1536), BF),
            pltpu.VMEM((4, 4, 64, 256), F32),
            pltpu.VMEM((4, 4, 4, 32, 128), F32),
            pltpu.VMEM((nx, 16, 128), BF),
            pltpu.VMEM((ny * nz, 16, 128), BF),
            pltpu.VMEM((ny * nz, 16, 128), BF),
            pltpu.VMEM((4, 4, 48, 128), F32),
            pltpu.SMEM((64,), jnp.int32),
            pltpu.SMEM((64,), jnp.int32),
            dma((6,)),
            dma((4,)),
            dma((3 * SEMS,)),
            dma((3 * SEMS,)),
            dma((nx,)),
            dma((nx,)),
            dma((ny * nz,)),
            dma((ny * nz,)),
        ],
        compiler_params=pltpu.CompilerParams(
            collective_id=0, has_side_effects=True, vmem_limit_bytes=60 * 1024 * 1024
        ),
    )(
        counts,
        near_offsets.T,
        far_offsets.transpose(2, 0, 1),
        charges,
        near_blocks,
        leaf_basis,
        transfer,
        coupling,
        coarse_coupling,
    )


def solution(mesh):
    sizes = (mesh.shape["gx"], mesh.shape["gy"], mesh.shape["gz"])
    spread = P("gx", "gy", "gz", None, None)
    in_specs = (spread, P("gx", "gy", "gz"), P(), P(), P(), P(), P(), P(), P())
    return jax.shard_map(
        functools.partial(body, sizes),
        mesh=mesh,
        in_specs=in_specs,
        out_specs=spread,
        check_vma=False,
    )
```
